128 devices in a mesh: stream: 4 (over x), tm: 32 (over z, y, core).
Axes of the slice: x: 4, y: 4, z: 4, core: 2. Of those that a mesh axis runs over, the one named last changes fastest.
Arguments:
- voltages: float32 [2, 16384, 4096], P(None, ('stream', 'tm')), parts along dimension 1, may hold values from -100 to 100
- taps: float32 [16, 4096], replicated, may hold values from -1.5 to 1.5
- flags: int32 [128], P('stream'), parts along dimension 0, may hold values from 0 to 1, as said below
Outputs:
- dynamic: float32 [4096, 4096], P('stream', 'tm'), parts along dimension 0
- kurtosis: float32 [16384], P(('stream', 'tm')), parts along dimension 0
- spectrum: float32 [16384], P(('stream', 'tm')), parts along dimension 0
The draws below stay inside these ranges and needn't reach their ends.
There are 4 independent parts, one for each index of `stream`. The reference program is written for one: setup_inputs(seed, part) draws one part's arguments, and reference() takes and returns one part's arrays. A program takes and returns all parts, laid end to end along the dimension named above; an argument that names none is the same for every part. Nothing has to cross between parts.
Inputs may be any that keep to these rules, and one draw needn't show every extreme that they name: `flags`: at least one and at most 16 blocks of a stream are flagged.
All inputs are finite; a program needn't handle non-finite values.
Results may differ from the reference program's by a relative error of at most 0.00016.
Values sent between devices are 32-bit elements; how exact they have to be, the bound alone decides.
A program may use at most 64 MiB of HBM per device.

```python
import jax
import jax.numpy as jnp
from jax import lax

CHANNEL_COUNT = 4096
TAPS = 16
FLAG_BLOCK = 128
SUMMED = 4
FRAMES = 4096
BLOCKS = 32


def draw_voltages(key, part):
    full_shape = (2, FRAMES, CHANNEL_COUNT)
    frame_place = jnp.arange(FRAMES, dtype=jnp.float32) / max(FRAMES - 1, 1)
    drift_gain = jnp.sqrt(1.0 + 2.0 * frame_place)[None, :, None]
    rough_part = jax.random.truncated_normal(key, -6.0, 6.0, full_shape, jnp.float32)
    values = rough_part * drift_gain
    return jnp.clip(values, -100.0, 100.0).astype(jnp.float32)


def draw_flags(key, part):
    ranking = jax.random.permutation(key, BLOCKS)
    flagged_count = jax.random.randint(jax.random.fold_in(key, 1), (), 1, BLOCKS // 2 + 1)
    return (ranking < flagged_count).astype(jnp.int32)


def normal_values(rng, extent, deviation, reach, held_as=jnp.bfloat16):
    return jnp.clip(deviation * jax.random.normal(rng, extent, jnp.float32), -reach, reach).astype(held_as)


def setup_inputs(seed: int = 0, part: int = 0) -> dict:
    key_of = jax.random.split(jax.random.key(seed), 4)
    part_splits = jax.random.split(jax.random.fold_in(key_of[3], part), 4)
    voltages = draw_voltages(jax.random.fold_in(jax.random.fold_in(key_of[3], part), 71), part)
    taps = normal_values(key_of[1], (TAPS, CHANNEL_COUNT), TAPS ** -0.5, 1.5, jnp.float32)
    flags = draw_flags(jax.random.fold_in(jax.random.fold_in(key_of[3], part), 71), part)
    return {"voltages": voltages, "taps": taps, "flags": flags}


def reference(voltages, taps, flags):
    frames = voltages.shape[1]
    padded = jnp.pad(voltages, ((0, 0), (TAPS - 1, 0), (0, 0)))
    filtered = jnp.zeros(voltages.shape, jnp.float32)
    for offset in range(TAPS):
        begin = TAPS - 1 - offset
        filtered = filtered + taps[offset][None, None, :] * padded[:, begin:begin + frames, :]
    spectra = jnp.fft.fft(filtered[0] + 1j * filtered[1], axis=-1)
    real_part = jnp.real(spectra)
    imag_part = jnp.imag(spectra)
    channel_powers = real_part * real_part + imag_part * imag_part
    mean_power = jnp.sum(channel_powers, axis=0)
    second_moment = jnp.sum(channel_powers * channel_powers, axis=0)
    kurtosis = ((frames + 1.0) / (frames - 1.0)) * (frames * second_moment / (mean_power * mean_power) - 1.0)
    clean_count = (1 - jnp.repeat(flags, FLAG_BLOCK)).astype(jnp.float32)
    group_sum = jnp.sum(channel_powers * clean_count[None, :])
    spectrum = CHANNEL_COUNT * clean_count * mean_power / group_sum
    integrated_power = jnp.sum(channel_powers.reshape(frames // SUMMED, SUMMED, CHANNEL_COUNT), axis=1)
    row_sum = jnp.dot(integrated_power, clean_count, precision=lax.Precision.HIGHEST)
    dynamic = CHANNEL_COUNT * clean_count[None, :] * integrated_power / row_sum[:, None]
    return dynamic, kurtosis, spectrum
```

```python
import functools

import jax
import jax.numpy as jnp
import ml_dtypes
import numpy as np
from jax import lax
from jax.experimental import pallas as pl
from jax.experimental.pallas import tpu as pltpu
from jax.sharding import PartitionSpec as P

J, L = 32, 128
TAPS = 16
CHUNK = 16
ROWS = CHUNK // 4
F32, BF16 = jnp.float32, jnp.bfloat16
MESH = pl.DeviceIdType.MESH


def split_table(table):
    high = table.astype(ml_dtypes.bfloat16)
    low = (table - high.astype(np.float64)).astype(ml_dtypes.bfloat16)
    return high, low


def complex_table(turns, steps):
    angle = 2.0 * np.pi * (turns % steps) / steps
    cosine, sine = np.cos(angle), np.sin(angle)
    return cosine, sine


def tables():
    q, j = np.arange(J)[:, None], np.arange(J)[None, :]
    cosine, sine = complex_table(q * j, J)
    outer = np.block([[cosine, sine], [-sine, cosine]])
    high, low = split_table(outer)
    outer_table = np.concatenate([high, high, low], 1)
    cosine, sine = complex_table(q * np.arange(L)[None, :], J * L)
    twist = np.stack([cosine, sine]).astype(np.float32)
    a, m = np.arange(L)[:, None], np.arange(L)[None, :]
    cosine, sine = complex_table(a * m, L)
    inner = np.block([[cosine, -sine], [sine, cosine]])
    return outer_table, twist, np.stack(split_table(inner))


def split(value):
    high = value.astype(BF16)
    low = (value - high.astype(F32)).astype(BF16)
    return high, low


def dot(a, b):
    return jnp.dot(a, b, preferred_element_type=F32)


def exchange(rows):
    lane = lax.broadcasted_iota(jnp.int32, rows[0].shape, 1)
    rows = list(rows)
    for bit in (2, 1):
        upper = (lane & bit) != 0
        for a in range(4):
            if a & bit:
                continue
            x, y = rows[a], rows[a + bit]
            rows[a] = jnp.where(upper, pltpu.roll(y, bit, 1), x)
            rows[a + bit] = jnp.where(upper, y, pltpu.roll(x, L - bit, 1))
    return rows


def owners_first(rows):
    return jnp.concatenate(exchange(rows), axis=0).T


def kernel(
    groups, frames,
    volt, taps, mask, outer, twist, inner,
    dyn, kurt, spec,
    vbuf, ybuf, tbuf, mbuf, moments, got,
    load_sem, halo_send, halo_recv, row_send, row_recv, mom_send, mom_recv,
):
    me = lax.axis_index("tm")
    chunks = frames // CHUNK
    blocks = frames // 8

    def load(piece, first, count):
        return pltpu.make_async_copy(
            volt.at[:, pl.ds(first, count)], vbuf.at[:, pl.ds(first + 2, count)], load_sem.at[piece]
        )

    load(0, blocks - 2, 2).start()
    load(1, 0, 4).start()
    for c in range(2, chunks - 1):
        load(c, 2 * c, 2).start()

    barrier = pltpu.get_barrier_semaphore()
    for d in range(1, groups):
        pl.semaphore_signal(barrier, 1, device_id={"tm": lax.rem(me + d, groups)}, device_id_type=MESH)

    def fir_part(c, s, jb, slot):
        t = [taps[pl.ds((k // 8) * 256 + jb * 64 + k % 8, 8, stride=8), :] for k in range(TAPS)]
        x = []
        for g in range(1, 2 * CHUNK):
            ref = vbuf.at[s, 2 * c + g // 8]
            x.append(ref[pl.ds(jb * 64 + g % 8, 8, stride=8), :])
        for f in range(CHUNK):
            total = t[0] * x[f + TAPS - 1]
            for k in range(1, TAPS):
                total = total + t[k] * x[f + TAPS - 1 - k]
            ybuf[slot, f, pl.ds(s * J + jb * 8, 8), :] = total

    def dft_part(quad, slot):
        cosine, sine = twist[0], twist[1]
        z = []
        for pair in range(2):
            f = quad * 4 + pair * 2
            y = jnp.concatenate([ybuf[slot, f], ybuf[slot, f + 1]], axis=1)
            high, low = split(y)
            o = dot(outer[...], jnp.concatenate([high, low, high], axis=0))
            for h in range(2):
                re, im = o[:J, h * L:(h + 1) * L], o[J:, h * L:(h + 1) * L]
                z.append(jnp.concatenate([re * cosine + im * sine, im * cosine - re * sine], axis=1))
        high, low = split(jnp.concatenate(z, axis=0))
        x = dot(high, inner[0]) + dot(low, inner[0]) + dot(high, inner[1])
        power = x[:, :L] * x[:, :L] + x[:, L:] * x[:, L:]
        p = [power[f * J:(f + 1) * J] for f in range(4)]
        row = (p[0] + p[1]) + (p[2] + p[3])
        moments[0] += row
        moments[1] += (p[0] * p[0] + p[1] * p[1]) + (p[2] * p[2] + p[3] * p[3])
        return row

    def send(src, dst, dest, send_sem, recv_sem):
        return pltpu.make_async_remote_copy(
            src, dst, send_sem, recv_sem, device_id={"tm": dest}, device_id_type=MESH
        )

    def finish_rows(c, rows):
        clean = mask[...]
        scaled = []
        for row in rows:
            part = jnp.sum(row, axis=0, keepdims=True) * clean
            total = jnp.sum(part, axis=1, keepdims=True)
            moments[2, pl.ds(0, 1), :] += part
            scaled.append(row * (clean * float(J * L)) * (1.0 / total))
        tbuf[c] = owners_first(scaled).reshape(groups, ROWS, L)
        for d in range(1, groups):
            dest = lax.rem(me + d, groups)
            send(tbuf.at[c, dest], dyn.at[me, c], dest, row_send, row_recv).start()
        dyn[me, c] = tbuf[c, me]

    moments[...] = jnp.zeros_like(moments)

    load(1, 0, 4).wait()
    for s in range(2):
        for jb in range(4):
            fir_part(1, s, jb, 1)
    load(0, blocks - 2, 2).wait()
    pl.semaphore_wait(barrier, groups - 1)

    def halo(dest):
        return send(
            vbuf.at[:, pl.ds(blocks, 2)], vbuf.at[:, pl.ds(0, 2)], dest, halo_send, halo_recv
        )

    following = lax.rem(me + 1, groups)

    @pl.when(me < groups - 1)
    def _():
        halo(following).start()

    @pl.loop(1, chunks - 1)
    def _(c):
        @pl.when(c < chunks - 2)
        def _():
            load(c + 1, 2 * (c + 1), 2).wait()

        rows = []
        for part in range(4):
            fir_part(c + 1, part // 2, part % 2 * 2, lax.rem(c + 1, 2))
            fir_part(c + 1, part // 2, part % 2 * 2 + 1, lax.rem(c + 1, 2))
            rows.append(dft_part(part, lax.rem(c, 2)))
        finish_rows(c, rows)

    finish_rows(chunks - 1, [dft_part(part, (chunks - 1) % 2) for part in range(4)])

    @pl.when(me > 0)
    def _():
        halo(following).wait_recv()

    @pl.when(me == 0)
    def _():
        vbuf[:, pl.ds(0, 2)] = jnp.zeros((2, 2, 256, L), F32)

    for s in range(2):
        for jb in range(4):
            fir_part(0, s, jb, 0)
    finish_rows(0, [dft_part(part, 0) for part in range(4)])

    local = jnp.sum(moments[2, pl.ds(0, 1), :], axis=1, keepdims=True)
    last = [moments[0], moments[1], jnp.broadcast_to(local, (J, L)), jnp.zeros((J, L), F32)]
    mbuf[...] = owners_first(last).reshape(groups, 4, L)
    for d in range(1, groups):
        dest = lax.rem(me + d, groups)
        send(mbuf.at[dest], got.at[me], dest, mom_send, mom_recv).start()
    got[me] = mbuf[me]

    everyone = pl.ds(0, groups - 1)
    send(mbuf.at[everyone], got.at[everyone], following, mom_send, mom_recv).wait_recv()
    sums = jnp.sum(got[...], axis=0)
    first, second, group = sums[0:1], sums[1:2], sums[2:3]
    count = float(frames * groups)
    kurt[...] = (count + 1.0) / (count - 1.0) * (count * second / (first * first) - 1.0)
    lane = lax.broadcasted_iota(jnp.int32, (1, L), 1)
    mine = jnp.sum(jnp.where(lane == 4 * me, mask[...], 0.0), axis=1, keepdims=True)
    spec[...] = float(J * L) * mine * first / group

    send(dyn.at[everyone], dyn.at[everyone], following, row_send, row_recv).wait()
    send(mbuf.at[everyone], got.at[everyone], following, mom_send, mom_recv).wait_send()

    @pl.when(me < groups - 1)
    def _():
        halo(following).wait_send()


def body(groups, voltages, taps, flags):
    frames = voltages.shape[1]
    chunks = frames // CHUNK
    volt = voltages.reshape(2, frames // 8, 8, J, L).transpose(0, 1, 3, 2, 4).reshape(2, frames // 8, 8 * J, L)
    tap = taps.reshape(TAPS // 8, 8, J, L).transpose(0, 2, 1, 3).reshape(TAPS * J, L)
    mask = jnp.broadcast_to((1 - flags).astype(F32)[:, None], (groups, 4)).reshape(1, L)
    outer, twist, inner = tables()
    vmem = pl.BlockSpec(memory_space=pltpu.VMEM)
    dyn, kurt, spec = pl.pallas_call(
        functools.partial(kernel, groups, frames),
        out_shape=(
            jax.ShapeDtypeStruct((groups, chunks, ROWS, L), F32),
            jax.ShapeDtypeStruct((1, L), F32),
            jax.ShapeDtypeStruct((1, L), F32),
        ),
        in_specs=[pl.BlockSpec(memory_space=pl.ANY)] + [vmem] * 5,
        out_specs=(vmem, vmem, vmem),
        scratch_shapes=[
            pltpu.VMEM((2, frames // 8 + 2, 8 * J, L), F32),
            pltpu.VMEM((2, CHUNK, 2 * J, L), F32),
            pltpu.VMEM((chunks, groups, ROWS, L), F32),
            pltpu.VMEM((groups, 4, L), F32),
            pltpu.VMEM((3, J, L), F32),
            pltpu.VMEM((groups, 4, L), F32),
            pltpu.SemaphoreType.DMA((chunks,)),
        ] + [pltpu.SemaphoreType.DMA] * 6,
        compiler_params=pltpu.CompilerParams(
            collective_id=0, has_side_effects=True, vmem_limit_bytes=40 * 1024 * 1024
        ),
    )(volt, tap, mask, jnp.asarray(outer), jnp.asarray(twist), jnp.asarray(inner))
    return dyn.reshape(groups * frames // 4, L), kurt.reshape(L), spec.reshape(L)


def solution(mesh):
    placed = (P(None, ("stream", "tm"), None), P(), P("stream"))
    return jax.shard_map(
        functools.partial(body, mesh.shape["tm"]),
        mesh=mesh,
        in_specs=placed,
        out_specs=(P("stream", "tm"), P(("stream", "tm")), P(("stream", "tm"))),
        check_vma=False,
    )
```

```python
import functools

import jax
import jax.numpy as jnp
import ml_dtypes
import numpy as np
from jax import lax
from jax.experimental import pallas as pl
from jax.experimental.pallas import tpu as pltpu
from jax.sharding import PartitionSpec as P

J, L = 32, 128
TAPS = 16
CHUNK = 32
F32, BF16 = jnp.float32, jnp.bfloat16
MESH = pl.DeviceIdType.MESH


def split_table(table):
    high = table.astype(ml_dtypes.bfloat16)
    low = (table - high.astype(np.float64)).astype(ml_dtypes.bfloat16)
    return high, low


def complex_table(turns, steps):
    angle = 2.0 * np.pi * (turns % steps) / steps
    cosine, sine = np.cos(angle), np.sin(angle)
    return cosine, sine


def tables():
    q, j = np.arange(J)[:, None], np.arange(J)[None, :]
    cosine, sine = complex_table(q * j, J)
    outer = np.block([[cosine, sine], [-sine, cosine]])
    high, low = split_table(outer)
    outer_table = np.concatenate([high, high, low], 1)
    cosine, sine = complex_table(q * np.arange(L)[None, :], J * L)
    twist = np.stack([cosine, sine]).astype(np.float32)
    a, m = np.arange(L)[:, None], np.arange(L)[None, :]
    cosine, sine = complex_table(a * m, L)
    inner = np.block([[cosine, -sine], [sine, cosine]])
    return outer_table, twist, np.stack(split_table(inner))


def split(value):
    high = value.astype(BF16)
    low = (value - high.astype(F32)).astype(BF16)
    return high, low


def dot(a, b):
    return jnp.dot(a, b, preferred_element_type=F32)


def exchange(rows):
    lane = lax.broadcasted_iota(jnp.int32, rows[0].shape, 1)
    rows = list(rows)
    for bit in (2, 1):
        upper = (lane & bit) != 0
        for a in range(4):
            if a & bit:
                continue
            x, y = rows[a], rows[a + bit]
            rows[a] = jnp.where(upper, pltpu.roll(y, bit, 1), x)
            rows[a + bit] = jnp.where(upper, y, pltpu.roll(x, L - bit, 1))
    return rows


def owners_first(rows):
    return jnp.concatenate(exchange(rows), axis=0).T


def kernel(
    groups, frames,
    volt, taps_in, flags_in, outer_in, twist_in, inner_in,
    dyn, kurt, spec,
    vbuf, taps, flags, outer, twist, inner, ybuf, zbuf, held, tbuf, mbuf, moments, got,
    load_sem, halo_send, halo_recv, row_send, row_recv, mom_send, mom_recv,
):
    me = lax.axis_index("tm")
    chunks = frames // CHUNK
    blocks = frames // 8
    span = CHUNK // 8

    def load(piece, part, first, count):
        return pltpu.make_async_copy(
            volt.at[part, pl.ds(first, count)], vbuf.at[part, pl.ds(first + 2, count)], load_sem.at[piece]
        )

    both = pl.ds(0, 2)
    loads = [
        pltpu.make_async_copy(taps_in, taps, load_sem.at[0]),
        load(1, 0, span - 2, span + 2),
        load(2, 1, span - 2, span + 2),
        load(3, both, blocks - 2, 2),
        pltpu.make_async_copy(outer_in, outer, load_sem.at[4]),
        pltpu.make_async_copy(twist_in, twist, load_sem.at[5]),
        pltpu.make_async_copy(inner_in, inner, load_sem.at[6]),
        pltpu.make_async_copy(flags_in, flags, load_sem.at[7]),
        load(8, both, 2 * span, blocks - 2 - 2 * span),
        load(9, both, 0, span - 2),
    ]
    for one in loads:
        one.start()

    barrier = pltpu.get_barrier_semaphore()
    for d in range(1, groups):
        pl.semaphore_signal(barrier, 1, device_id={"tm": lax.rem(me + d, groups)}, device_id_type=MESH)

    def fir(c, s):
        @pl.loop(0, J // 8)
        def _(jb):
            def tap(k):
                return taps[pl.ds(jb * 64 + ((k // 8) * 256 + k % 8), 8, stride=8), :]

            def sample(g):
                return vbuf.at[s, span * c + (g + 16) // 8][pl.ds(jb * 64 + (g + 16) % 8, 8, stride=8), :]

            half = TAPS // 2
            even_taps = [tap(2 * i) for i in range(half)]
            odd_taps = [tap(2 * i + 1) for i in range(half)]
            sum_taps = [a + b for a, b in zip(even_taps, odd_taps)]

            def run(h, x):
                total = h[0] * x[half - 1]
                for i in range(1, half):
                    total = total + h[i] * x[half - 1 - i]
                return total

            even = [sample(2 * n) for n in range(1 - half, 0)]
            odd = [sample(2 * n + 1) for n in range(-half, 0)]
            both_x = [a + b for a, b in zip(even, odd[1:])]
            before = run(odd_taps, odd)
            for n in range(CHUNK // 2):
                even, odd = (even + [sample(2 * n)])[-half:], odd[1:] + [sample(2 * n + 1)]
                both_x = (both_x + [even[-1] + odd[-1]])[-half:]
                a, b, ab = run(even_taps, even), run(odd_taps, odd), run(sum_taps, both_x)
                place = pl.ds(pl.multiple_of(s * J + jb * 8, 8), 8)
                ybuf[2 * n, place, :] = a + before
                ybuf[2 * n + 1, place, :] = ab - (a + b)
                before = b

    def first_stage(part):
        cosine, sine = twist[0], twist[1]
        for pair in range(4):
            f = part * 8 + pair * 2
            y = jnp.concatenate([ybuf[f], ybuf[f + 1]], axis=1)
            high, low = split(y)
            o = dot(outer[...], jnp.concatenate([high, low, high], axis=0))
            for h in range(2):
                re, im = o[:J, h * L:(h + 1) * L], o[J:, h * L:(h + 1) * L]
                z = jnp.concatenate([re * cosine + im * sine, im * cosine - re * sine], axis=1)
                place = pl.ds((pair * 2 + h) * J, J)
                zbuf[part, 0, place, :], zbuf[part, 1, place, :] = split(z)

    def second_stage(part):
        high, low = zbuf[part, 0], zbuf[part, 1]
        x = dot(high, inner[0]) + dot(low, inner[0]) + dot(high, inner[1])
        power = x[:, :L] * x[:, :L] + x[:, L:] * x[:, L:]
        for r in range(2):
            p = [power[(4 * r + f) * J:(4 * r + f + 1) * J] for f in range(4)]
            row = (p[0] + p[1]) + (p[2] + p[3])
            moments[0] += row
            moments[1] += (p[0] * p[0] + p[1] * p[1]) + (p[2] * p[2] + p[3] * p[3])
            held[part * 2 + r] = row

    def send(src, dst, dest, send_sem, recv_sem):
        return pltpu.make_async_remote_copy(
            src, dst, send_sem, recv_sem, device_id={"tm": dest}, device_id_type=MESH
        )

    def clean_lanes():
        block = lax.broadcasted_iota(jnp.int32, (groups, L), 0)
        lane = lax.broadcasted_iota(jnp.int32, (groups, L), 1)
        spread = jnp.where(lane // 4 == block, 1.0, 0.0)
        clean = jnp.broadcast_to(1.0 - flags[...].astype(F32), (8, groups))
        return dot(clean.astype(BF16), spread.astype(BF16))[0:1]

    def finish_rows(c, side):
        clean = moments[2, pl.ds(8, 1), :]
        scaled = []
        for a in range(4):
            row = held[side * 4 + a]
            part = jnp.sum(row, axis=0, keepdims=True) * clean
            total = jnp.sum(part, axis=1, keepdims=True)
            moments[2, pl.ds(0, 1), :] += part
            scaled.append(row * (clean * float(J * L)) * (1.0 / total))
        tbuf[c, side] = owners_first(scaled).reshape(groups, 4, L)

    def send_rows(c):
        for d in range(1, groups):
            dest = lax.rem(me + d, groups)
            send(tbuf.at[c, both, dest], dyn.at[me, c], dest, row_send, row_recv).start()
        dyn[me, c] = tbuf[c, both, me]

    def halo(dest):
        return send(
            vbuf.at[:, pl.ds(blocks, 2)], vbuf.at[:, pl.ds(0, 2)], dest, halo_send, halo_recv
        )

    following = lax.rem(me + 1, groups)
    moments[...] = jnp.zeros_like(moments)

    loads[0].wait()
    loads[1].wait()
    fir(1, 0)
    loads[2].wait()
    fir(1, 1)
    loads[3].wait()
    pl.semaphore_wait(barrier, groups - 1)

    @pl.when(me < groups - 1)
    def _():
        halo(following).start()

    for piece in range(4, 10):
        loads[piece].wait()
    moments[2, pl.ds(8, 1), :] = clean_lanes()

    def spectra(c, earlier):
        first_stage(0)
        if earlier is not None:
            finish_rows(earlier, 1)
        first_stage(1)
        second_stage(0)
        first_stage(2)
        second_stage(1)
        if earlier is not None:
            send_rows(earlier)
        finish_rows(c, 0)
        first_stage(3)
        second_stage(2)
        second_stage(3)

    spectra(1, None)

    @pl.loop(2, chunks + 1)
    def _(i):
        c = lax.rem(i, chunks)

        @pl.when(i == chunks)
        def _():
            @pl.when(me > 0)
            def _():
                halo(following).wait_recv()

            @pl.when(me == 0)
            def _():
                vbuf[:, pl.ds(0, 2)] = jnp.zeros((2, 2, 8 * J, L), F32)

        fir(c, 0)
        fir(c, 1)
        spectra(c, i - 1)

    finish_rows(0, 1)
    send_rows(0)

    local = jnp.sum(moments[2, pl.ds(0, 1), :], axis=1, keepdims=True)
    last = [moments[0], moments[1], jnp.broadcast_to(local, (J, L)), jnp.zeros((J, L), F32)]
    mbuf[...] = owners_first(last).reshape(groups, 4, L)
    for d in range(1, groups):
        dest = lax.rem(me + d, groups)
        send(mbuf.at[dest], got.at[me], dest, mom_send, mom_recv).start()
    got[me] = mbuf[me]

    everyone = pl.ds(0, groups - 1)
    send(mbuf.at[everyone], got.at[everyone], following, mom_send, mom_recv).wait_recv()
    sums = jnp.sum(got[...], axis=0)
    first, second, group = sums[0:1], sums[1:2], sums[2:3]
    count = float(frames * groups)
    kurt[...] = (count + 1.0) / (count - 1.0) * (count * second / (first * first) - 1.0)
    lane = lax.broadcasted_iota(jnp.int32, (1, L), 1)
    mine = jnp.sum(jnp.where(lane == 4 * me, moments[2, pl.ds(8, 1), :], 0.0), axis=1, keepdims=True)
    spec[...] = float(J * L) * mine * first / group

    send(dyn.at[everyone], dyn.at[everyone], following, row_send, row_recv).wait()
    send(mbuf.at[everyone], got.at[everyone], following, mom_send, mom_recv).wait_send()

    @pl.when(me < groups - 1)
    def _():
        halo(following).wait_send()


def body(groups, voltages, taps, flags):
    frames = voltages.shape[1]
    chunks = frames // CHUNK
    volt = voltages.reshape(2, frames // 8, 8, J, L).transpose(0, 1, 3, 2, 4).reshape(2, frames // 8, 8 * J, L)
    tap = taps.reshape(TAPS // 8, 8, J, L).transpose(0, 2, 1, 3).reshape(TAPS * J, L)
    outer, twist, inner = tables()
    vmem = pl.BlockSpec(memory_space=pltpu.VMEM)
    dyn, kurt, spec = pl.pallas_call(
        functools.partial(kernel, groups, frames),
        out_shape=(
            jax.ShapeDtypeStruct((groups, chunks, CHUNK // 16, 4, L), F32),
            jax.ShapeDtypeStruct((1, L), F32),
            jax.ShapeDtypeStruct((1, L), F32),
        ),
        in_specs=[pl.BlockSpec(memory_space=pl.ANY)] * 6,
        out_specs=(vmem, vmem, vmem),
        scratch_shapes=[
            pltpu.VMEM((2, frames // 8 + 2, 8 * J, L), F32),
            pltpu.VMEM((TAPS * J, L), F32),
            pltpu.VMEM((1, groups), jnp.int32),
            pltpu.VMEM(outer.shape, BF16),
            pltpu.VMEM(twist.shape, F32),
            pltpu.VMEM(inner.shape, BF16),
            pltpu.VMEM((CHUNK, 2 * J, L), F32),
            pltpu.VMEM((CHUNK // 8, 2, 8 * J, 2 * L), BF16),
            pltpu.VMEM((CHUNK // 4, J, L), F32),
            pltpu.VMEM((chunks, CHUNK // 16, groups, 4, L), F32),
            pltpu.VMEM((groups, 4, L), F32),
            pltpu.VMEM((3, J, L), F32),
            pltpu.VMEM((groups, 4, L), F32),
            pltpu.SemaphoreType.DMA((10,)),
        ] + [pltpu.SemaphoreType.DMA] * 6,
        compiler_params=pltpu.CompilerParams(
            collective_id=0, has_side_effects=True, vmem_limit_bytes=63 * 1024 * 1024
        ),
    )(volt, tap, flags.reshape(1, groups), jnp.asarray(outer), jnp.asarray(twist), jnp.asarray(inner))
    return dyn.reshape(groups * frames // 4, L), kurt.reshape(L), spec.reshape(L)


def solution(mesh):
    placed = (P(None, ("stream", "tm"), None), P(), P("stream"))
    return jax.shard_map(
        functools.partial(body, mesh.shape["tm"]),
        mesh=mesh,
        in_specs=placed,
        out_specs=(P("stream", "tm"), P(("stream", "tm")), P(("stream", "tm"))),
        check_vma=False,
    )
```

```python
import functools

import jax
import jax.numpy as jnp
import ml_dtypes
import numpy as np
from jax import lax
from jax.experimental import pallas as pl
from jax.experimental.pallas import tpu as pltpu
from jax.sharding import PartitionSpec as P

J, L = 32, 128
TAPS = 16
CHUNK = 32
FAR_FIRST = sorted(
    ((dz, dy) for dz in range(4) for dy in range(4)), key=lambda d: -(min(d[0], 4 - d[0]) + min(d[1], 4 - d[1]))
)
F32, BF16 = jnp.float32, jnp.bfloat16
MESH = pl.DeviceIdType.MESH


def split_table(table):
    high = table.astype(ml_dtypes.bfloat16)
    low = (table - high.astype(np.float64)).astype(ml_dtypes.bfloat16)
    return high, low


def complex_table(turns, steps):
    angle = 2.0 * np.pi * (turns % steps) / steps
    cosine, sine = np.cos(angle), np.sin(angle)
    return cosine, sine


def tables():
    q, j = np.arange(J)[:, None], np.arange(J)[None, :]
    cosine, sine = complex_table(q * j, J)
    outer = np.block([[cosine, sine], [-sine, cosine]])
    high, low = split_table(outer)
    outer_table = np.concatenate([high, high, low], 1)
    cosine, sine = complex_table(q * np.arange(L)[None, :], J * L)
    twist = np.stack([cosine, sine]).astype(np.float32)
    a, m = np.arange(L)[:, None], np.arange(L)[None, :]
    cosine, sine = complex_table(a * m, L)
    inner = np.block([[cosine, -sine], [sine, cosine]])
    return outer_table, twist, np.stack(split_table(inner))


def split(value):
    high = value.astype(BF16)
    low = (value - high.astype(F32)).astype(BF16)
    return high, low


def dot(a, b):
    return jnp.dot(a, b, preferred_element_type=F32)


def exchange(rows):
    lane = lax.broadcasted_iota(jnp.int32, rows[0].shape, 1)
    rows = list(rows)
    for bit in (2, 1):
        upper = (lane & bit) != 0
        for a in range(4):
            if a & bit:
                continue
            x, y = rows[a], rows[a + bit]
            rows[a] = jnp.where(upper, pltpu.roll(y, bit, 1), x)
            rows[a + bit] = jnp.where(upper, y, pltpu.roll(x, L - bit, 1))
    return rows


def owners_first(rows):
    return jnp.concatenate(exchange(rows), axis=0).T


def kernel(
    groups, frames,
    volt, taps_in, flags_in, outer_in, twist_in, inner_in,
    dyn, kurt, spec,
    vbuf, taps, flags, outer, twist, inner, half_taps, xbuf, ybuf, zbuf, held, wide, narrow, final, moments, got,
    load_sem, ready, halo_send, halo_recv, row_send, row_recv, fin_send, fin_recv,
):
    me = lax.axis_index("tm")
    blocks = frames // 8
    half = TAPS // 2
    both = pl.ds(0, 2)
    following, preceding = lax.rem(me + 1, groups), lax.rem(me + groups - 1, groups)

    def load(piece, part, first, count):
        return pltpu.make_async_copy(
            volt.at[part, pl.ds(first, count)], vbuf.at[part, pl.ds(first + 2, count)], load_sem.at[piece]
        )

    loads = [
        pltpu.make_async_copy(taps_in, taps, load_sem.at[0]),
        load(1, both, blocks - 2, 2),
        load(2, 0, 0, 6),
        load(3, 1, 0, 6),
        pltpu.make_async_copy(outer_in, outer, load_sem.at[4]),
        pltpu.make_async_copy(twist_in, twist, load_sem.at[5]),
        pltpu.make_async_copy(inner_in, inner, load_sem.at[6]),
        pltpu.make_async_copy(flags_in, flags, load_sem.at[7]),
        load(8, both, 6, 4),
        load(9, both, 10, 4),
    ]
    for one in loads:
        one.start()

    def signal(semaphore, dest):
        pl.semaphore_signal(semaphore, 1, device_id={"tm": dest}, device_id_type=MESH)

    barrier = pltpu.get_barrier_semaphore()
    signal(barrier, following)
    signal(barrier, preceding)

    def spread(level):
        step = 1 if level == 0 else 2 ** (level - 1)
        signal(ready.at[level], lax.rem(me + step, groups))
        signal(ready.at[level], lax.rem(me + groups - step, groups))

    def known(level):
        pl.semaphore_wait(ready.at[level], 2)

    def send(src, dst, dest, send_sem, recv_sem):
        return pltpu.make_async_remote_copy(
            src, dst, send_sem, recv_sem, device_id={"tm": dest}, device_id_type=MESH
        )

    def halo(s):
        return send(
            vbuf.at[s, pl.ds(blocks, 2)], vbuf.at[s, pl.ds(0, 2)], following, halo_send.at[s], halo_recv.at[s]
        )

    column, core = me // 2 % 4, me % 2
    plane = me // 8
    others = [
        lax.rem(plane + dz, 4) * 8 + lax.rem(column + dy, 4) * 2 + lax.rem(core + dc, 2)
        for dz, dy in FAR_FIRST for dc in (0, 1) if (dz, dy, dc) != (0, 0, 0)
    ]

    def split_taps():
        for jb in range(J // 8):
            t = [taps[pl.ds(jb * 64 + ((k // 8) * 256 + k % 8), 8, stride=8), :] for k in range(TAPS)]
            for i in range(half):
                half_taps[jb, i] = t[2 * i]
                half_taps[jb, half + i] = t[2 * i + 1]
                half_taps[jb, 2 * half + i] = t[2 * i] + t[2 * i + 1]

    def fir(first, count, s):
        pairs = count // 2
        base = first // 8

        @pl.loop(0, J // 8)
        def _(jb):
            def sample(g):
                return vbuf.at[s, base + (g + 16) // 8][pl.ds(jb * 64 + (g + 16) % 8, 8, stride=8), :]

            def run(h, x):
                total = h[0] * x[half - 1]
                for i in range(1, half):
                    total = total + h[i] * x[half - 1 - i]
                return total

            h = [half_taps[jb, i] for i in range(half)]
            x = [sample(2 * n) for n in range(1 - half, 0)]
            for n in range(1 - half, 0):
                xbuf[0, n + half] = x[n + half - 1]
            for n in range(pairs):
                x = (x + [sample(2 * n)])[-half:]
                xbuf[0, n + half] = x[-1]
                xbuf[1, n] = run(h, x)

            place = pl.ds(pl.multiple_of(s * J + jb * 8, 8), 8)
            h = [half_taps[jb, half + i] for i in range(half)]
            x = [sample(2 * n + 1) for n in range(-half, 0)]
            for n in range(1 - half, 0):
                xbuf[3, n + half] = x[n + half] + xbuf[0, n + half]
            before = run(h, x)
            for n in range(pairs):
                x = x[1:] + [sample(2 * n + 1)]
                xbuf[3, n + half] = x[-1] + xbuf[0, n + half]
                a, b = xbuf[1, n], run(h, x)
                ybuf[2 * n, place, :] = a + before
                xbuf[2, n] = a + b
                before = b

            h = [half_taps[jb, 2 * half + i] for i in range(half)]
            x = [xbuf[3, n + half] for n in range(1 - half, 0)]
            for n in range(pairs):
                x = (x + [xbuf[3, n + half]])[-half:]
                ybuf[2 * n + 1, place, :] = run(h, x) - xbuf[2, n]

    def first_stage(part):
        cosine, sine = twist[0], twist[1]
        for pair in range(4):
            f = part * 8 + pair * 2
            y = jnp.concatenate([ybuf[f], ybuf[f + 1]], axis=1)
            high, low = split(y)
            o = dot(outer[...], jnp.concatenate([high, low, high], axis=0))
            for h in range(2):
                re, im = o[:J, h * L:(h + 1) * L], o[J:, h * L:(h + 1) * L]
                z = jnp.concatenate([re * cosine + im * sine, im * cosine - re * sine], axis=1)
                place = pl.ds((pair * 2 + h) * J, J)
                zbuf[part, 0, place, :], zbuf[part, 1, place, :] = split(z)

    def second_stage(part):
        high, low = zbuf[part, 0], zbuf[part, 1]
        x = dot(high, inner[0]) + dot(low, inner[0]) + dot(high, inner[1])
        power = x[:, :L] * x[:, :L] + x[:, L:] * x[:, L:]
        for r in range(2):
            p = [power[(4 * r + f) * J:(4 * r + f + 1) * J] for f in range(4)]
            row = (p[0] + p[1]) + (p[2] + p[3])
            moments[0] += row
            moments[1] += (p[0] * p[0] + p[1] * p[1]) + (p[2] * p[2] + p[3] * p[3])
            held[part * 2 + r] = row

    def clean_lanes():
        block = lax.broadcasted_iota(jnp.int32, (groups, L), 0)
        lane = lax.broadcasted_iota(jnp.int32, (groups, L), 1)
        spread_out = jnp.where(lane // 4 == block, 1.0, 0.0)
        clean = jnp.broadcast_to(1.0 - flags[...].astype(F32), (8, groups))
        return dot(clean.astype(BF16), spread_out.astype(BF16))[0:1]

    def finish_rows(side, target):
        clean = moments[2, pl.ds(8, 1), :]
        scaled = []
        for a in range(4):
            row = held[side * 4 + a]
            part = jnp.sum(row, axis=0, keepdims=True) * clean
            total = jnp.sum(part, axis=1, keepdims=True)
            moments[2, pl.ds(0, 1), :] += part
            scaled.append(row * (clean * float(J * L)) * (1.0 / total))
        target[...] = owners_first(scaled).reshape(groups, 4, L)

    def send_wide(g):
        for dest in others:
            send(wide.at[g, dest], dyn.at[me, pl.ds(1 + 2 * g, 2)], dest, row_send, row_recv).start()

    def send_narrow():
        for dest in others:
            send(narrow.at[dest], dyn.at[me, 7], dest, row_send, row_recv).start()

    def spectra(parts, pending):
        first_stage(0)
        for action in pending:
            action()
        for part in range(1, parts):
            first_stage(part)
            second_stage(part - 1)
        second_stage(parts - 1)

    moments[...] = jnp.zeros_like(moments)

    loads[0].wait()
    split_taps()
    loads[1].wait()
    pl.semaphore_wait(barrier, 2)

    @pl.when(me < groups - 1)
    def _():
        halo(0).start()
        halo(1).start()

    spread(0)
    loads[2].wait()
    fir(16, 32, 0)
    known(0)
    spread(1)
    loads[3].wait()
    fir(16, 32, 1)
    known(1)
    spread(2)
    for piece in range(4, 10):
        loads[piece].wait()
    moments[2, pl.ds(8, 1), :] = clean_lanes()
    spectra(4, [])
    finish_rows(0, wide.at[0, :, 0])
    finish_rows(1, wide.at[0, :, 1])
    known(2)
    spread(3)
    fir(48, 32, 0)
    known(3)
    spread(4)
    fir(48, 32, 1)
    known(4)
    send_wide(0)
    spectra(4, [])
    finish_rows(0, wide.at[1, :, 0])
    finish_rows(1, wide.at[1, :, 1])
    send_wide(1)
    fir(80, 32, 0)
    fir(80, 32, 1)
    spectra(4, [])
    finish_rows(0, wide.at[2, :, 0])
    finish_rows(1, wide.at[2, :, 1])
    send_wide(2)
    fir(112, 16, 0)
    fir(112, 16, 1)
    spectra(2, [])
    finish_rows(0, narrow)
    send_narrow()

    for s in range(2):
        @pl.when(me > 0)
        def _():
            halo(s).wait_recv()

        @pl.when(me == 0)
        def _():
            vbuf[s, pl.ds(0, 2)] = jnp.zeros((2, 8 * J, L), F32)

        fir(0, 16, s)
    spectra(2, [])
    finish_rows(0, final.at[:, 0])

    local = jnp.sum(moments[2, pl.ds(0, 1), :], axis=1, keepdims=True)
    last = [moments[0], moments[1], jnp.broadcast_to(local, (J, L)), jnp.zeros((J, L), F32)]
    final[:, 1] = owners_first(last).reshape(groups, 4, L)
    for dest in others:
        send(final.at[dest], got.at[me], dest, fin_send, fin_recv).start()
    got[me] = final[me]
    for g in range(3):
        dyn[me, pl.ds(1 + 2 * g, 2)] = wide[g, me]
    dyn[me, 7] = narrow[me]

    everyone = pl.ds(0, groups - 1)
    send(final.at[everyone], got.at[everyone], following, fin_send, fin_recv).wait_recv()
    dyn[:, 0] = got[:, 0]
    sums = jnp.sum(got[:, 1], axis=0)
    first, second, group = sums[0:1], sums[1:2], sums[2:3]
    count = float(frames * groups)
    kurt[...] = (count + 1.0) / (count - 1.0) * (count * second / (first * first) - 1.0)
    lane = lax.broadcasted_iota(jnp.int32, (1, L), 1)
    mine = jnp.sum(jnp.where(lane == 4 * me, moments[2, pl.ds(8, 1), :], 0.0), axis=1, keepdims=True)
    spec[...] = float(J * L) * mine * first / group

    units = dyn.at[everyone, pl.ds(1, 7)]
    send(units, units, following, row_send, row_recv).wait()
    send(final.at[everyone], got.at[everyone], following, fin_send, fin_recv).wait_send()

    @pl.when(me < groups - 1)
    def _():
        halo(0).wait_send()
        halo(1).wait_send()


def body(groups, voltages, taps, flags):
    frames = voltages.shape[1]
    volt = voltages.reshape(2, frames // 8, 8, J, L).transpose(0, 1, 3, 2, 4).reshape(2, frames // 8, 8 * J, L)
    tap = taps.reshape(TAPS // 8, 8, J, L).transpose(0, 2, 1, 3).reshape(TAPS * J, L)
    outer, twist, inner = tables()
    vmem = pl.BlockSpec(memory_space=pltpu.VMEM)
    half = TAPS // 2
    operands = (volt, tap, flags.reshape(1, groups), jnp.asarray(outer), jnp.asarray(twist), jnp.asarray(inner))
    dyn, kurt, spec = pl.pallas_call(
        functools.partial(kernel, groups, frames),
        out_shape=(
            jax.ShapeDtypeStruct((groups, frames // 16, 4, L), F32),
            jax.ShapeDtypeStruct((1, L), F32),
            jax.ShapeDtypeStruct((1, L), F32),
        ),
        in_specs=[pl.BlockSpec(memory_space=pltpu.HBM)] * 6,
        out_specs=(vmem, vmem, vmem),
        scratch_shapes=[
            pltpu.VMEM((2, frames // 8 + 2, 8 * J, L), F32),
            pltpu.VMEM((TAPS * J, L), F32),
            pltpu.VMEM((1, groups), jnp.int32),
            pltpu.VMEM(outer.shape, BF16),
            pltpu.VMEM(twist.shape, F32),
            pltpu.VMEM(inner.shape, BF16),
            pltpu.VMEM((J // 8, 3 * half, 8, L), F32),
            pltpu.VMEM((4, CHUNK // 2 + half, 8, L), F32),
            pltpu.VMEM((CHUNK, 2 * J, L), F32),
            pltpu.VMEM((CHUNK // 8, 2, 8 * J, 2 * L), BF16),
            pltpu.VMEM((CHUNK // 4, J, L), F32),
            pltpu.VMEM((3, groups, 2, 4, L), F32),
            pltpu.VMEM((groups, 4, L), F32),
            pltpu.VMEM((groups, 2, 4, L), F32),
            pltpu.VMEM((3, J, L), F32),
            pltpu.VMEM((groups, 2, 4, L), F32),
            pltpu.SemaphoreType.DMA((10,)),
            pltpu.SemaphoreType.REGULAR((5,)),
            pltpu.SemaphoreType.DMA((2,)),
            pltpu.SemaphoreType.DMA((2,)),
        ] + [pltpu.SemaphoreType.DMA] * 4,
        compiler_params=pltpu.CompilerParams(
            collective_id=0, has_side_effects=True, vmem_limit_bytes=40 * 1024 * 1024
        ),
    )(*(pltpu.with_memory_space_constraint(x, pltpu.HBM) for x in operands))
    return dyn.reshape(groups * frames // 4, L), kurt.reshape(L), spec.reshape(L)


def solution(mesh):
    placed = (P(None, ("stream", "tm"), None), P(), P("stream"))
    return jax.shard_map(
        functools.partial(body, mesh.shape["tm"]),
        mesh=mesh,
        in_specs=placed,
        out_specs=(P("stream", "tm"), P(("stream", "tm")), P(("stream", "tm"))),
        check_vma=False,
    )
```

```python
import functools

import jax
import jax.numpy as jnp
import ml_dtypes
import numpy as np
from jax import lax
from jax.experimental import pallas as pl
from jax.experimental.pallas import tpu as pltpu
from jax.sharding import PartitionSpec as P

J, L = 32, 128
TAPS = 16
CHUNK = 32
FAR_FIRST = sorted(
    ((dz, dy) for dz in range(4) for dy in range(4)), key=lambda d: -(min(d[0], 4 - d[0]) + min(d[1], 4 - d[1]))
)
F32, BF16 = jnp.float32, jnp.bfloat16
MESH = pl.DeviceIdType.MESH


def split_table(table):
    high = table.astype(ml_dtypes.bfloat16)
    low = (table - high.astype(np.float64)).astype(ml_dtypes.bfloat16)
    return high, low


def complex_table(turns, steps):
    angle = 2.0 * np.pi * (turns % steps) / steps
    cosine, sine = np.cos(angle), np.sin(angle)
    return cosine, sine


def tables():
    q, j = np.arange(J)[:, None], np.arange(J)[None, :]
    cosine, sine = complex_table(q * j, J)
    outer = np.block([[cosine, sine], [-sine, cosine]])
    high, low = split_table(outer)
    outer_table = np.concatenate([high, high, low], 1)
    cosine, sine = complex_table(q * np.arange(L)[None, :], J * L)
    twist = np.stack([cosine, sine]).astype(np.float32)
    a, m = np.arange(L)[:, None], np.arange(L)[None, :]
    cosine, sine = complex_table(a * m, L)
    inner = np.block([[cosine, -sine], [sine, cosine]])
    return outer_table, twist, np.stack(split_table(inner))


def split(value):
    high = value.astype(BF16)
    low = (value - high.astype(F32)).astype(BF16)
    return high, low


def dot(a, b):
    return jnp.dot(a, b, preferred_element_type=F32)


def exchange(rows):
    lane = lax.broadcasted_iota(jnp.int32, rows[0].shape, 1)
    rows = list(rows)
    for bit in (2, 1):
        upper = (lane & bit) != 0
        for a in range(4):
            if a & bit:
                continue
            x, y = rows[a], rows[a + bit]
            rows[a] = jnp.where(upper, pltpu.roll(y, bit, 1), x)
            rows[a + bit] = jnp.where(upper, y, pltpu.roll(x, L - bit, 1))
    return rows


def owners_first(rows):
    return jnp.concatenate(exchange(rows), axis=0).T


def kernel(
    groups, frames,
    volt, taps_in, flags_in, outer_in, twist_in, inner_in,
    dyn, got, mine,
    vbuf, taps, flags, outer, twist, inner, half_taps, xbuf, ybuf, zbuf, held, wide, narrow, final, moments,
    load_sem, halo_send, halo_recv, row_send, row_recv, fin_send, fin_recv,
):
    me = lax.axis_index("tm")
    blocks = frames // 8
    half = TAPS // 2
    both = pl.ds(0, 2)
    following = lax.rem(me + 1, groups)

    def load(piece, part, first, count):
        return pltpu.make_async_copy(
            volt.at[part, pl.ds(first, count)], vbuf.at[part, pl.ds(first + 2, count)], load_sem.at[piece]
        )

    loads = [
        pltpu.make_async_copy(taps_in, taps, load_sem.at[0]),
        load(1, both, blocks - 2, 2),
        load(2, 0, 0, 6),
        load(3, 1, 0, 6),
        pltpu.make_async_copy(outer_in, outer, load_sem.at[4]),
        pltpu.make_async_copy(twist_in, twist, load_sem.at[5]),
        pltpu.make_async_copy(inner_in, inner, load_sem.at[6]),
        pltpu.make_async_copy(flags_in, flags, load_sem.at[7]),
        load(8, both, 6, 4),
        load(9, both, 10, 4),
    ]
    for one in loads:
        one.start()

    def signal(semaphore, dest):
        pl.semaphore_signal(semaphore, 1, device_id={"tm": dest}, device_id_type=MESH)

    barrier = pltpu.get_barrier_semaphore()
    for d in range(1, groups):
        signal(barrier, lax.rem(me + d, groups))

    def send(src, dst, dest, send_sem, recv_sem):
        return pltpu.make_async_remote_copy(
            src, dst, send_sem, recv_sem, device_id={"tm": dest}, device_id_type=MESH
        )

    def halo(s):
        return send(
            vbuf.at[s, pl.ds(blocks, 2)], vbuf.at[s, pl.ds(0, 2)], following, halo_send.at[s], halo_recv.at[s]
        )

    column, core = me // 2 % 4, me % 2
    plane = me // 8
    others = [
        lax.rem(plane + dz, 4) * 8 + lax.rem(column + dy, 4) * 2 + lax.rem(core + dc, 2)
        for dz, dy in FAR_FIRST for dc in (0, 1) if (dz, dy, dc) != (0, 0, 0)
    ]

    def split_taps():
        for jb in range(J // 8):
            t = [taps[pl.ds(jb * 64 + ((k // 8) * 256 + k % 8), 8, stride=8), :] for k in range(TAPS)]
            for i in range(half):
                half_taps[jb, i] = t[2 * i]
                half_taps[jb, half + i] = t[2 * i + 1]
                half_taps[jb, 2 * half + i] = t[2 * i] + t[2 * i + 1]

    def fir(first, count, s, jb, slot):
        pairs = count // 2
        keep = xbuf.at[jb % 2]

        def sample(g):
            return vbuf.at[s, (first + g + 16) // 8][pl.ds(jb * 64 + (g + 16) % 8, 8, stride=8), :]

        def run(h, x):
            total = h[0] * x[half - 1]
            for i in range(1, half):
                total = total + h[i] * x[half - 1 - i]
            return total

        h = [half_taps[jb, i] for i in range(half)]
        x = [sample(2 * n) for n in range(1 - half, 0)]
        for n in range(1 - half, 0):
            keep[0, n + half] = x[n + half - 1]
        for n in range(pairs):
            x = (x + [sample(2 * n)])[-half:]
            keep[0, n + half] = x[-1]
            keep[1, n] = run(h, x)

        place = pl.ds(s * J + jb * 8, 8)
        h = [half_taps[jb, half + i] for i in range(half)]
        x = [sample(2 * n + 1) for n in range(-half, 0)]
        for n in range(1 - half, 0):
            keep[3, n + half] = x[n + half] + keep[0, n + half]
        before = run(h, x)
        for n in range(pairs):
            x = x[1:] + [sample(2 * n + 1)]
            keep[3, n + half] = x[-1] + keep[0, n + half]
            a, b = keep[1, n], run(h, x)
            ybuf[slot, 2 * n, place, :] = a + before
            keep[2, n] = a + b
            before = b

        h = [half_taps[jb, 2 * half + i] for i in range(half)]
        x = [keep[3, n + half] for n in range(1 - half, 0)]
        for n in range(pairs):
            x = (x + [keep[3, n + half]])[-half:]
            ybuf[slot, 2 * n + 1, place, :] = run(h, x) - keep[2, n]

    def first_stage(part, slot):
        cosine, sine = twist[0], twist[1]
        for pair in range(4):
            f = part * 8 + pair * 2
            y = jnp.concatenate([ybuf[slot, f], ybuf[slot, f + 1]], axis=1)
            high, low = split(y)
            o = dot(outer[...], jnp.concatenate([high, low, high], axis=0))
            for h in range(2):
                re, im = o[:J, h * L:(h + 1) * L], o[J:, h * L:(h + 1) * L]
                z = jnp.concatenate([re * cosine + im * sine, im * cosine - re * sine], axis=1)
                place = pl.ds((pair * 2 + h) * J, J)
                zbuf[part, 0, place, :], zbuf[part, 1, place, :] = split(z)

    def second_stage(part, slot):
        high, low = zbuf[part, 0], zbuf[part, 1]
        x = dot(high, inner[0]) + dot(low, inner[0]) + dot(high, inner[1])
        power = x[:, :L] * x[:, :L] + x[:, L:] * x[:, L:]
        for r in range(2):
            p = [power[(4 * r + f) * J:(4 * r + f + 1) * J] for f in range(4)]
            row = (p[0] + p[1]) + (p[2] + p[3])
            moments[0] += row
            moments[1] += (p[0] * p[0] + p[1] * p[1]) + (p[2] * p[2] + p[3] * p[3])
            held[slot, part * 2 + r] = row

    def clean_lanes():
        block = lax.broadcasted_iota(jnp.int32, (groups, L), 0)
        lane = lax.broadcasted_iota(jnp.int32, (groups, L), 1)
        spread_out = jnp.where(lane // 4 == block, 1.0, 0.0)
        clean = jnp.broadcast_to(1.0 - flags[...].astype(F32), (8, groups))
        return dot(clean.astype(BF16), spread_out.astype(BF16))[0:1]

    def finish_rows(slot, side, target):
        clean = moments[2, pl.ds(8, 1), :]
        scaled = []
        for a in range(4):
            row = held[slot, side * 4 + a]
            part = jnp.sum(row, axis=0, keepdims=True) * clean
            total = jnp.sum(part, axis=1, keepdims=True)
            moments[2, pl.ds(0, 1), :] += part
            scaled.append(row * (clean * float(J * L)) * (1.0 / total))
        target[...] = owners_first(scaled).reshape(groups, 4, L)

    def send_wide(g):
        for dest in others:
            send(wide.at[g, dest], dyn.at[me, pl.ds(1 + 2 * g, 2)], dest, row_send, row_recv).start()

    def send_narrow():
        for dest in others:
            send(narrow.at[dest], dyn.at[me, 7], dest, row_send, row_recv).start()

    pieces = [(s, jb) for s in range(2) for jb in range(J // 8)]

    def stages(parts, slot):
        order = [functools.partial(first_stage, 0, slot)]
        for part in range(1, parts):
            order.append(functools.partial(first_stage, part, slot))
            order.append(functools.partial(second_stage, part - 1, slot))
        return order + [functools.partial(second_stage, parts - 1, slot)]

    def interleave(*lists):
        keyed = [((n + 0.5) / len(one), k, action) for k, one in enumerate(lists) for n, action in enumerate(one)]
        for _, _, action in sorted(keyed, key=lambda entry: entry[:2]):
            action()

    def filters(first, count, slot):
        return [functools.partial(fir, first, count, s, jb, slot) for s, jb in pieces]

    moments[...] = jnp.zeros_like(moments)

    loads[0].wait()
    split_taps()
    loads[2].wait()
    for action in filters(16, 32, 0)[:4]:
        action()
    loads[3].wait()
    for action in filters(16, 32, 0)[4:]:
        action()
    loads[1].wait()
    pl.semaphore_wait(barrier, groups - 1)

    @pl.when(me < groups - 1)
    def _():
        halo(0).start()
        halo(1).start()

    for piece in range(4, 10):
        loads[piece].wait()
    moments[2, pl.ds(8, 1), :] = clean_lanes()

    def finish(g, side):
        return functools.partial(finish_rows, g % 2, side, wide.at[g, :, side])

    interleave(filters(48, 32, 1), stages(4, 0))
    interleave(
        filters(80, 32, 0),
        stages(4, 1),
        [finish(0, 0), finish(0, 1), functools.partial(send_wide, 0)],
    )
    interleave(
        filters(112, 16, 1),
        stages(4, 0),
        [finish(1, 0), finish(1, 1), functools.partial(send_wide, 1)],
    )
    interleave(stages(2, 1), [finish(2, 0), finish(2, 1), functools.partial(send_wide, 2)])
    finish_rows(1, 0, narrow)
    send_narrow()

    for s in range(2):
        @pl.when(me > 0)
        def _():
            halo(s).wait_recv()

        @pl.when(me == 0)
        def _():
            vbuf[s, pl.ds(0, 2)] = jnp.zeros((2, 8 * J, L), F32)

        for action in filters(0, 16, 0)[4 * s:4 * s + 4]:
            action()
    interleave(stages(2, 0))
    finish_rows(0, 0, final.at[:, 0])

    local = jnp.sum(moments[2, pl.ds(0, 1), :], axis=1, keepdims=True)
    last = [moments[0], moments[1], jnp.broadcast_to(local, (J, L)), jnp.zeros((J, L), F32)]
    final[:, 1] = owners_first(last).reshape(groups, 4, L)
    for dest in others:
        send(final.at[dest], got.at[me], dest, fin_send, fin_recv).start()
    got[me] = final[me]
    for g in range(3):
        dyn[me, pl.ds(1 + 2 * g, 2)] = wide[g, me]
    dyn[me, 7] = narrow[me]

    everyone = pl.ds(0, groups - 1)
    send(final.at[everyone], got.at[everyone], following, fin_send, fin_recv).wait_recv()
    lane = lax.broadcasted_iota(jnp.int32, (1, L), 1)
    own = jnp.sum(jnp.where(lane == 4 * me, moments[2, pl.ds(8, 1), :], 0.0), axis=1, keepdims=True)
    mine[...] = jnp.broadcast_to(own, (1, L))

    units = dyn.at[everyone, pl.ds(1, 7)]
    send(units, units, following, row_send, row_recv).wait()
    send(final.at[everyone], got.at[everyone], following, fin_send, fin_recv).wait_send()

    @pl.when(me < groups - 1)
    def _():
        halo(0).wait_send()
        halo(1).wait_send()


def deliver(count, dyn, got, mine, rows, kurt, spec, kbuf, sbuf, sem):
    later = pltpu.make_async_copy(dyn.at[:, pl.ds(1, 7)], rows.at[:, pl.ds(1, 7)], sem.at[0])
    early = pltpu.make_async_copy(got.at[:, 0], rows.at[:, 0], sem.at[1])
    later.start()
    early.start()
    sums = jnp.sum(got[:, 1], axis=0)
    first, second, group = sums[0:1], sums[1:2], sums[2:3]
    kbuf[...] = (count + 1.0) / (count - 1.0) * (count * second / (first * first) - 1.0)
    sbuf[...] = float(J * L) * mine[...] * first / group
    small = [pltpu.make_async_copy(kbuf, kurt, sem.at[2]), pltpu.make_async_copy(sbuf, spec, sem.at[3])]
    for one in small:
        one.start()
    for one in small:
        one.wait()
    later.wait()
    early.wait()


def body(groups, voltages, taps, flags):
    frames = voltages.shape[1]
    volt = voltages.reshape(2, frames // 8, 8, J, L).transpose(0, 1, 3, 2, 4).reshape(2, frames // 8, 8 * J, L)
    tap = taps.reshape(TAPS // 8, 8, J, L).transpose(0, 2, 1, 3).reshape(TAPS * J, L)
    outer, twist, inner = tables()
    vmem = pl.BlockSpec(memory_space=pltpu.VMEM)
    half = TAPS // 2
    operands = (volt, tap, flags.reshape(1, groups), jnp.asarray(outer), jnp.asarray(twist), jnp.asarray(inner))
    received = pl.pallas_call(
        functools.partial(kernel, groups, frames),
        out_shape=(
            jax.ShapeDtypeStruct((groups, frames // 16, 4, L), F32),
            jax.ShapeDtypeStruct((groups, 2, 4, L), F32),
            jax.ShapeDtypeStruct((1, L), F32),
        ),
        in_specs=[pl.BlockSpec(memory_space=pltpu.HBM)] * 6,
        out_specs=(vmem, vmem, vmem),
        scratch_shapes=[
            pltpu.VMEM((2, frames // 8 + 2, 8 * J, L), F32),
            pltpu.VMEM((TAPS * J, L), F32),
            pltpu.VMEM((1, groups), jnp.int32),
            pltpu.VMEM(outer.shape, BF16),
            pltpu.VMEM(twist.shape, F32),
            pltpu.VMEM(inner.shape, BF16),
            pltpu.VMEM((J // 8, 3 * half, 8, L), F32),
            pltpu.VMEM((2, 4, CHUNK // 2 + half, 8, L), F32),
            pltpu.VMEM((2, CHUNK, 2 * J, L), F32),
            pltpu.VMEM((CHUNK // 8, 2, 8 * J, 2 * L), BF16),
            pltpu.VMEM((2, CHUNK // 4, J, L), F32),
            pltpu.VMEM((3, groups, 2, 4, L), F32),
            pltpu.VMEM((groups, 4, L), F32),
            pltpu.VMEM((groups, 2, 4, L), F32),
            pltpu.VMEM((3, J, L), F32),
            pltpu.SemaphoreType.DMA((10,)),
            pltpu.SemaphoreType.DMA((2,)),
            pltpu.SemaphoreType.DMA((2,)),
        ] + [pltpu.SemaphoreType.DMA] * 4,
        compiler_params=pltpu.CompilerParams(
            collective_id=0, has_side_effects=True, vmem_limit_bytes=40 * 1024 * 1024
        ),
    )(*(pltpu.with_memory_space_constraint(x, pltpu.HBM) for x in operands))
    hbm = pl.BlockSpec(memory_space=pltpu.HBM)
    dyn, kurt, spec = pl.pallas_call(
        functools.partial(deliver, float(frames * groups)),
        out_shape=(
            jax.ShapeDtypeStruct((groups, frames // 16, 4, L), F32),
            jax.ShapeDtypeStruct((1, L), F32),
            jax.ShapeDtypeStruct((1, L), F32),
        ),
        in_specs=[vmem] * 3,
        out_specs=(hbm, hbm, hbm),
        scratch_shapes=[pltpu.VMEM((1, L), F32), pltpu.VMEM((1, L), F32), pltpu.SemaphoreType.DMA((4,))],
        compiler_params=pltpu.CompilerParams(vmem_limit_bytes=4 * 1024 * 1024),
    )(*received)
    return dyn.reshape(groups * frames // 4, L), kurt.reshape(L), spec.reshape(L)


def solution(mesh):
    placed = (P(None, ("stream", "tm"), None), P(), P("stream"))
    return jax.shard_map(
        functools.partial(body, mesh.shape["tm"]),
        mesh=mesh,
        in_specs=placed,
        out_specs=(P("stream", "tm"), P(("stream", "tm")), P(("stream", "tm"))),
        check_vma=False,
    )
```

```python
import functools

import jax
import jax.numpy as jnp
import ml_dtypes
import numpy as np
from jax import lax
from jax.experimental import pallas as pl
from jax.experimental.pallas import tpu as pltpu
from jax.sharding import PartitionSpec as P

J, L = 32, 128
TAPS = 16
CHUNK = 32
FAR_FIRST = sorted(
    ((dz, dy) for dz in range(4) for dy in range(4)), key=lambda d: -(min(d[0], 4 - d[0]) + min(d[1], 4 - d[1]))
)
F32, BF16 = jnp.float32, jnp.bfloat16
MESH = pl.DeviceIdType.MESH


def split_table(table):
    high = table.astype(ml_dtypes.bfloat16)
    low = (table - high.astype(np.float64)).astype(ml_dtypes.bfloat16)
    return high, low


def complex_table(turns, steps):
    angle = 2.0 * np.pi * (turns % steps) / steps
    cosine, sine = np.cos(angle), np.sin(angle)
    return cosine, sine


def tables():
    q, j = np.arange(J)[:, None], np.arange(J)[None, :]
    cosine, sine = complex_table(q * j, J)
    outer = np.block([[cosine, sine], [-sine, cosine]])
    high, low = split_table(outer)
    outer_table = np.concatenate([high, high, low], 1)
    cosine, sine = complex_table(q * np.arange(L)[None, :], J * L)
    twist = np.stack([cosine, sine]).astype(np.float32)
    a, m = np.arange(L)[:, None], np.arange(L)[None, :]
    cosine, sine = complex_table(a * m, L)
    inner = np.block([[cosine, -sine], [sine, cosine]])
    return outer_table, twist, np.stack(split_table(inner))


def split(value):
    high = value.astype(BF16)
    low = (value - high.astype(F32)).astype(BF16)
    return high, low


def dot(a, b):
    return jnp.dot(a, b, preferred_element_type=F32)


def exchange(rows):
    lane = lax.broadcasted_iota(jnp.int32, rows[0].shape, 1)
    rows = list(rows)
    for bit in (2, 1):
        upper = (lane & bit) != 0
        for a in range(4):
            if a & bit:
                continue
            x, y = rows[a], rows[a + bit]
            rows[a] = jnp.where(upper, pltpu.roll(y, bit, 1), x)
            rows[a + bit] = jnp.where(upper, y, pltpu.roll(x, L - bit, 1))
    return rows


def owners_first(rows):
    return jnp.concatenate(exchange(rows), axis=0).T


def kernel(
    groups, frames,
    volt, taps_in, flags_in, outer_in, twist_in, inner_in,
    dyn, got, mine,
    vbuf, taps, flags, outer, twist, inner, half_taps, xbuf, ybuf, zbuf, held, wide, narrow, final, moments,
    load_sem, ready, halo_send, halo_recv, row_send, row_recv, fin_send, fin_recv,
):
    me = lax.axis_index("tm")
    blocks = frames // 8
    half = TAPS // 2
    both = pl.ds(0, 2)
    following = lax.rem(me + 1, groups)

    def load(piece, part, first, count):
        return pltpu.make_async_copy(
            volt.at[part, pl.ds(first, count)], vbuf.at[part, pl.ds(first + 2, count)], load_sem.at[piece]
        )

    loads = [
        pltpu.make_async_copy(taps_in, taps, load_sem.at[0]),
        load(1, both, blocks - 2, 2),
        load(2, 0, 0, 6),
        load(3, 1, 0, 6),
        pltpu.make_async_copy(outer_in, outer, load_sem.at[4]),
        pltpu.make_async_copy(twist_in, twist, load_sem.at[5]),
        pltpu.make_async_copy(inner_in, inner, load_sem.at[6]),
        pltpu.make_async_copy(flags_in, flags, load_sem.at[7]),
        load(8, both, 6, 4),
        load(9, both, 10, 4),
    ]
    for one in loads:
        one.start()

    def signal(semaphore, dest):
        pl.semaphore_signal(semaphore, 1, device_id={"tm": dest}, device_id_type=MESH)

    barrier = pltpu.get_barrier_semaphore()
    column, core, plane = me // 2 % 4, me % 2, me // 8
    line = [plane * 8 + lax.rem(me + d, 8) for d in range(1, 8)]
    across = [lax.rem(me + 8 * d, groups) for d in range(1, 4)]
    for dest in line + across:
        signal(barrier, dest)
    ends = (lax.rem(me, 8) == 7, lax.rem(me, 8) == 0)

    @pl.when(ends[0])
    def _():
        signal(barrier, following)

    @pl.when(ends[1])
    def _():
        signal(barrier, lax.rem(me + groups - 1, groups))

    def near_entered():
        place = lax.rem(me, 8)
        pl.semaphore_wait(barrier, 10 + lax.div(place, 7) + lax.div(7 - place, 7))

    def send(src, dst, dest, send_sem, recv_sem):
        return pltpu.make_async_remote_copy(
            src, dst, send_sem, recv_sem, device_id={"tm": dest}, device_id_type=MESH
        )

    def halo(s):
        return send(
            vbuf.at[s, pl.ds(blocks, 2)], vbuf.at[s, pl.ds(0, 2)], following, halo_send.at[s], halo_recv.at[s]
        )

    others = [
        lax.rem(plane + dz, 4) * 8 + lax.rem(column + dy, 4) * 2 + lax.rem(core + dc, 2)
        for dz, dy in FAR_FIRST for dc in (0, 1) if (dz, dy, dc) != (0, 0, 0)
    ]

    def split_taps():
        for jb in range(J // 8):
            t = [taps[pl.ds(jb * 64 + ((k // 8) * 256 + k % 8), 8, stride=8), :] for k in range(TAPS)]
            for i in range(half):
                half_taps[jb, i] = t[2 * i]
                half_taps[jb, half + i] = t[2 * i + 1]
                half_taps[jb, 2 * half + i] = t[2 * i] + t[2 * i + 1]

    def fir(first, count, s, jb, slot):
        pairs = count // 2
        keep = xbuf.at[jb % 2]

        def sample(g):
            return vbuf.at[s, (first + g + 16) // 8][pl.ds(jb * 64 + (g + 16) % 8, 8, stride=8), :]

        def run(h, x):
            total = h[0] * x[half - 1]
            for i in range(1, half):
                total = total + h[i] * x[half - 1 - i]
            return total

        h = [half_taps[jb, i] for i in range(half)]
        x = [sample(2 * n) for n in range(1 - half, 0)]
        for n in range(1 - half, 0):
            keep[0, n + half] = x[n + half - 1]
        for n in range(pairs):
            x = (x + [sample(2 * n)])[-half:]
            keep[0, n + half] = x[-1]
            keep[1, n] = run(h, x)

        place = pl.ds(s * J + jb * 8, 8)
        h = [half_taps[jb, half + i] for i in range(half)]
        x = [sample(2 * n + 1) for n in range(-half, 0)]
        for n in range(1 - half, 0):
            keep[3, n + half] = x[n + half] + keep[0, n + half]
        before = run(h, x)
        for n in range(pairs):
            x = x[1:] + [sample(2 * n + 1)]
            keep[3, n + half] = x[-1] + keep[0, n + half]
            a, b = keep[1, n], run(h, x)
            ybuf[slot, 2 * n, place, :] = a + before
            keep[2, n] = a + b
            before = b

        h = [half_taps[jb, 2 * half + i] for i in range(half)]
        x = [keep[3, n + half] for n in range(1 - half, 0)]
        for n in range(pairs):
            x = (x + [keep[3, n + half]])[-half:]
            ybuf[slot, 2 * n + 1, place, :] = run(h, x) - keep[2, n]

    def first_stage(part, slot):
        cosine, sine = twist[0], twist[1]
        for pair in range(4):
            f = part * 8 + pair * 2
            y = jnp.concatenate([ybuf[slot, f], ybuf[slot, f + 1]], axis=1)
            high, low = split(y)
            o = dot(outer[...], jnp.concatenate([high, low, high], axis=0))
            for h in range(2):
                re, im = o[:J, h * L:(h + 1) * L], o[J:, h * L:(h + 1) * L]
                z = jnp.concatenate([re * cosine + im * sine, im * cosine - re * sine], axis=1)
                place = pl.ds((pair * 2 + h) * J, J)
                zbuf[part, 0, place, :], zbuf[part, 1, place, :] = split(z)

    def second_stage(part, slot):
        high, low = zbuf[part, 0], zbuf[part, 1]
        x = dot(high, inner[0]) + dot(low, inner[0]) + dot(high, inner[1])
        power = x[:, :L] * x[:, :L] + x[:, L:] * x[:, L:]
        for r in range(2):
            p = [power[(4 * r + f) * J:(4 * r + f + 1) * J] for f in range(4)]
            row = (p[0] + p[1]) + (p[2] + p[3])
            moments[0] += row
            moments[1] += (p[0] * p[0] + p[1] * p[1]) + (p[2] * p[2] + p[3] * p[3])
            held[slot, part * 2 + r] = row

    def clean_lanes():
        block = lax.broadcasted_iota(jnp.int32, (groups, L), 0)
        lane = lax.broadcasted_iota(jnp.int32, (groups, L), 1)
        spread_out = jnp.where(lane // 4 == block, 1.0, 0.0)
        clean = jnp.broadcast_to(1.0 - flags[...].astype(F32), (8, groups))
        return dot(clean.astype(BF16), spread_out.astype(BF16))[0:1]

    def finish_rows(slot, side, target):
        clean = moments[2, pl.ds(8, 1), :]
        scaled = []
        for a in range(4):
            row = held[slot, side * 4 + a]
            part = jnp.sum(row, axis=0, keepdims=True) * clean
            total = jnp.sum(part, axis=1, keepdims=True)
            moments[2, pl.ds(0, 1), :] += part
            scaled.append(row * (clean * float(J * L)) * (1.0 / total))
        target[...] = owners_first(scaled).reshape(groups, 4, L)

    def in_turn(one, count):
        def some(dests):
            for dest in dests:
                one(dest).start()

        return [functools.partial(some, others[n::count]) for n in range(count)]

    def send_wide(g):
        return in_turn(
            lambda dest: send(wide.at[g, dest], dyn.at[me, pl.ds(1 + 2 * g, 2)], dest, row_send, row_recv), 8
        )

    def send_narrow(count):
        return in_turn(lambda dest: send(narrow.at[dest], dyn.at[me, 7], dest, row_send, row_recv), count)

    pieces = [(s, jb) for s in range(2) for jb in range(J // 8)]

    def stages(parts, slot):
        order = [functools.partial(first_stage, 0, slot)]
        for part in range(1, parts):
            order.append(functools.partial(first_stage, part, slot))
            order.append(functools.partial(second_stage, part - 1, slot))
        return order + [functools.partial(second_stage, parts - 1, slot)]

    def interleave(*lists):
        keyed = [((n + 0.5) / len(one), k, action) for k, one in enumerate(lists) for n, action in enumerate(one)]
        for _, _, action in sorted(keyed, key=lambda entry: entry[:2]):
            action()

    def filters(first, count, slot):
        return [functools.partial(fir, first, count, s, jb, slot) for s, jb in pieces]

    moments[...] = jnp.zeros_like(moments)

    loads[0].wait()
    split_taps()
    loads[1].wait()
    near_entered()

    @pl.when(me < groups - 1)
    def _():
        halo(0).start()
        halo(1).start()

    for dest in across:
        signal(ready, dest)
    loads[2].wait()
    for action in filters(16, 32, 0)[:4]:
        action()
    loads[3].wait()
    for action in filters(16, 32, 0)[4:]:
        action()
    for piece in range(4, 10):
        loads[piece].wait()
    moments[2, pl.ds(8, 1), :] = clean_lanes()

    def finish(g, side):
        return functools.partial(finish_rows, g % 2, side, wide.at[g, :, side])

    interleave(stages(4, 0))
    interleave(filters(48, 32, 1))
    pl.semaphore_wait(ready, 3)
    interleave(stages(4, 1), [finish(0, 0), finish(0, 1)])
    interleave(filters(80, 32, 0), send_wide(0))
    interleave(stages(4, 0), [finish(1, 0), finish(1, 1)])
    interleave(filters(112, 16, 1), send_wide(1))
    interleave(stages(2, 1), [finish(2, 0), finish(2, 1)])
    interleave(send_wide(2), [functools.partial(finish_rows, 1, 0, narrow)])
    for action in send_narrow(1):
        action()

    for s in range(2):
        @pl.when(me > 0)
        def _():
            halo(s).wait_recv()

        @pl.when(me == 0)
        def _():
            vbuf[s, pl.ds(0, 2)] = jnp.zeros((2, 8 * J, L), F32)

        for action in filters(0, 16, 0)[4 * s:4 * s + 4]:
            action()
    interleave(stages(2, 0))
    finish_rows(0, 0, final.at[:, 0])

    local = jnp.sum(moments[2, pl.ds(0, 1), :], axis=1, keepdims=True)
    last = [moments[0], moments[1], jnp.broadcast_to(local, (J, L)), jnp.zeros((J, L), F32)]
    final[:, 1] = owners_first(last).reshape(groups, 4, L)
    for dest in others:
        send(final.at[dest], got.at[me], dest, fin_send, fin_recv).start()
    got[me] = final[me]
    for g in range(3):
        dyn[me, pl.ds(1 + 2 * g, 2)] = wide[g, me]
    dyn[me, 7] = narrow[me]

    everyone = pl.ds(0, groups - 1)
    send(final.at[everyone], got.at[everyone], following, fin_send, fin_recv).wait_recv()
    lane = lax.broadcasted_iota(jnp.int32, (1, L), 1)
    own = jnp.sum(jnp.where(lane == 4 * me, moments[2, pl.ds(8, 1), :], 0.0), axis=1, keepdims=True)
    mine[...] = jnp.broadcast_to(own, (1, L))

    units = dyn.at[everyone, pl.ds(1, 7)]
    send(units, units, following, row_send, row_recv).wait()
    send(final.at[everyone], got.at[everyone], following, fin_send, fin_recv).wait_send()

    @pl.when(me < groups - 1)
    def _():
        halo(0).wait_send()
        halo(1).wait_send()


def deliver(count, dyn, got, mine, rows, kurt, spec, kbuf, sbuf, sem):
    later = pltpu.make_async_copy(dyn.at[:, pl.ds(1, 7)], rows.at[:, pl.ds(1, 7)], sem.at[0])
    early = pltpu.make_async_copy(got.at[:, 0], rows.at[:, 0], sem.at[1])
    later.start()
    early.start()
    sums = jnp.sum(got[:, 1], axis=0)
    first, second, group = sums[0:1], sums[1:2], sums[2:3]
    kbuf[...] = (count + 1.0) / (count - 1.0) * (count * second / (first * first) - 1.0)
    sbuf[...] = float(J * L) * mine[...] * first / group
    small = [pltpu.make_async_copy(kbuf, kurt, sem.at[2]), pltpu.make_async_copy(sbuf, spec, sem.at[3])]
    for one in small:
        one.start()
    for one in small:
        one.wait()
    later.wait()
    early.wait()


def body(groups, voltages, taps, flags):
    frames = voltages.shape[1]
    volt = voltages.reshape(2, frames // 8, 8, J, L).transpose(0, 1, 3, 2, 4).reshape(2, frames // 8, 8 * J, L)
    tap = taps.reshape(TAPS // 8, 8, J, L).transpose(0, 2, 1, 3).reshape(TAPS * J, L)
    outer, twist, inner = tables()
    vmem = pl.BlockSpec(memory_space=pltpu.VMEM)
    half = TAPS // 2
    operands = (volt, tap, flags.reshape(1, groups), jnp.asarray(outer), jnp.asarray(twist), jnp.asarray(inner))
    received = pl.pallas_call(
        functools.partial(kernel, groups, frames),
        out_shape=(
            jax.ShapeDtypeStruct((groups, frames // 16, 4, L), F32),
            jax.ShapeDtypeStruct((groups, 2, 4, L), F32),
            jax.ShapeDtypeStruct((1, L), F32),
        ),
        in_specs=[pl.BlockSpec(memory_space=pltpu.HBM)] * 6,
        out_specs=(vmem, vmem, vmem),
        scratch_shapes=[
            pltpu.VMEM((2, frames // 8 + 2, 8 * J, L), F32),
            pltpu.VMEM((TAPS * J, L), F32),
            pltpu.VMEM((1, groups), jnp.int32),
            pltpu.VMEM(outer.shape, BF16),
            pltpu.VMEM(twist.shape, F32),
            pltpu.VMEM(inner.shape, BF16),
            pltpu.VMEM((J // 8, 3 * half, 8, L), F32),
            pltpu.VMEM((2, 4, CHUNK // 2 + half, 8, L), F32),
            pltpu.VMEM((2, CHUNK, 2 * J, L), F32),
            pltpu.VMEM((CHUNK // 8, 2, 8 * J, 2 * L), BF16),
            pltpu.VMEM((2, CHUNK // 4, J, L), F32),
            pltpu.VMEM((3, groups, 2, 4, L), F32),
            pltpu.VMEM((groups, 4, L), F32),
            pltpu.VMEM((groups, 2, 4, L), F32),
            pltpu.VMEM((3, J, L), F32),
            pltpu.SemaphoreType.DMA((10,)),
            pltpu.SemaphoreType.REGULAR,
            pltpu.SemaphoreType.DMA((2,)),
            pltpu.SemaphoreType.DMA((2,)),
        ] + [pltpu.SemaphoreType.DMA] * 4,
        compiler_params=pltpu.CompilerParams(
            collective_id=0, has_side_effects=True, vmem_limit_bytes=40 * 1024 * 1024
        ),
    )(*(pltpu.with_memory_space_constraint(x, pltpu.HBM) for x in operands))
    hbm = pl.BlockSpec(memory_space=pltpu.HBM)
    dyn, kurt, spec = pl.pallas_call(
        functools.partial(deliver, float(frames * groups)),
        out_shape=(
            jax.ShapeDtypeStruct((groups, frames // 16, 4, L), F32),
            jax.ShapeDtypeStruct((1, L), F32),
            jax.ShapeDtypeStruct((1, L), F32),
        ),
        in_specs=[vmem] * 3,
        out_specs=(hbm, hbm, hbm),
        scratch_shapes=[pltpu.VMEM((1, L), F32), pltpu.VMEM((1, L), F32), pltpu.SemaphoreType.DMA((4,))],
        compiler_params=pltpu.CompilerParams(vmem_limit_bytes=4 * 1024 * 1024),
    )(*received)
    return dyn.reshape(groups * frames // 4, L), kurt.reshape(L), spec.reshape(L)


def solution(mesh):
    placed = (P(None, ("stream", "tm"), None), P(), P("stream"))
    return jax.shard_map(
        functools.partial(body, mesh.shape["tm"]),
        mesh=mesh,
        in_specs=placed,
        out_specs=(P("stream", "tm"), P(("stream", "tm")), P(("stream", "tm"))),
        check_vma=False,
    )
```

```python
import functools

import jax
import jax.numpy as jnp
import ml_dtypes
import numpy as np
from jax import lax
from jax.experimental import pallas as pl
from jax.experimental.pallas import tpu as pltpu
from jax.sharding import PartitionSpec as P

J, L = 32, 128
TAPS = 16
CHUNK = 32
FAR_FIRST = sorted(
    ((dz, dy) for dz in range(4) for dy in range(4)), key=lambda d: -(min(d[0], 4 - d[0]) + min(d[1], 4 - d[1]))
)
F32, BF16 = jnp.float32, jnp.bfloat16
MESH = pl.DeviceIdType.MESH


def split_table(table):
    high = table.astype(ml_dtypes.bfloat16)
    low = (table - high.astype(np.float64)).astype(ml_dtypes.bfloat16)
    return high, low


def complex_table(turns, steps):
    angle = 2.0 * np.pi * (turns % steps) / steps
    cosine, sine = np.cos(angle), np.sin(angle)
    return cosine, sine


def tables():
    q, j = np.arange(J)[:, None], np.arange(J)[None, :]
    cosine, sine = complex_table(q * j, J)
    outer = np.block([[cosine, sine], [-sine, cosine]])
    high, low = split_table(outer)
    outer_table = np.concatenate([high, high, low], 1)
    cosine, sine = complex_table(q * np.arange(L)[None, :], J * L)
    twist = np.stack([cosine, sine]).astype(np.float32)
    a, m = np.arange(L)[:, None], np.arange(L)[None, :]
    cosine, sine = complex_table(a * m, L)
    inner = np.block([[cosine, -sine], [sine, cosine]])
    return outer_table, twist, np.stack(split_table(inner))


def split(value):
    high = value.astype(BF16)
    low = (value - high.astype(F32)).astype(BF16)
    return high, low


def dot(a, b):
    return jnp.dot(a, b, preferred_element_type=F32)


def exchange(rows):
    lane = lax.broadcasted_iota(jnp.int32, rows[0].shape, 1)
    rows = list(rows)
    for bit in (2, 1):
        upper = (lane & bit) != 0
        for a in range(4):
            if a & bit:
                continue
            x, y = rows[a], rows[a + bit]
            rows[a] = jnp.where(upper, pltpu.roll(y, bit, 1), x)
            rows[a + bit] = jnp.where(upper, y, pltpu.roll(x, L - bit, 1))
    return rows


def owners_first(rows, scale=None):
    rows = exchange(rows)
    if scale is not None:
        rows = [row * scale for row in rows]
    return jnp.concatenate(rows, axis=0).T


def kernel(
    groups, frames,
    volt, taps_in, flags_in, outer_in, twist_in, inner_in,
    dyn, got, mine,
    vbuf, taps, flags, outer, twist, inner, tap_sums, xbuf, ybuf, zbuf, held, wide, late, final, moments,
    load_sem, ready, halo_send, halo_recv, row_send, row_recv, fin_send, fin_recv,
):
    me = lax.axis_index("tm")
    blocks = frames // 8
    quarter = TAPS // 4
    both = pl.ds(0, 2)
    following = lax.rem(me + 1, groups)

    def load(piece, part, first, count):
        return pltpu.make_async_copy(
            volt.at[part, pl.ds(first, count)], vbuf.at[part, pl.ds(first + 2, count)], load_sem.at[piece]
        )

    loads = [
        pltpu.make_async_copy(taps_in, taps, load_sem.at[0]),
        load(1, both, blocks - 2, 2),
        load(2, 0, 0, 6),
        load(3, 1, 0, 6),
        pltpu.make_async_copy(outer_in, outer, load_sem.at[4]),
        pltpu.make_async_copy(twist_in, twist, load_sem.at[5]),
        pltpu.make_async_copy(inner_in, inner, load_sem.at[6]),
        pltpu.make_async_copy(flags_in, flags, load_sem.at[7]),
        load(8, both, 6, 4),
        load(9, both, 10, 4),
    ]
    for one in loads:
        one.start()

    def signal(semaphore, dest):
        pl.semaphore_signal(semaphore, 1, device_id={"tm": dest}, device_id_type=MESH)

    barrier = pltpu.get_barrier_semaphore()
    column, core, plane = me // 2 % 4, me % 2, me // 8
    line = [plane * 8 + lax.rem(me + d, 8) for d in range(1, 8)]
    across = [lax.rem(me + 8 * d, groups) for d in range(1, 4)]
    for dest in line + across:
        signal(barrier, dest)
    ends = (lax.rem(me, 8) == 7, lax.rem(me, 8) == 0)

    @pl.when(ends[0])
    def _():
        signal(barrier, following)

    @pl.when(ends[1])
    def _():
        signal(barrier, lax.rem(me + groups - 1, groups))

    def near_entered():
        place = lax.rem(me, 8)
        pl.semaphore_wait(barrier, 10 + lax.div(place, 7) + lax.div(7 - place, 7))

    def send(src, dst, dest, send_sem, recv_sem):
        return pltpu.make_async_remote_copy(
            src, dst, send_sem, recv_sem, device_id={"tm": dest}, device_id_type=MESH
        )

    def halo(s):
        return send(
            vbuf.at[s, pl.ds(blocks, 2)], vbuf.at[s, pl.ds(0, 2)], following, halo_send.at[s], halo_recv.at[s]
        )

    others = [
        lax.rem(plane + dz, 4) * 8 + lax.rem(column + dy, 4) * 2 + lax.rem(core + dc, 2)
        for dz, dy in FAR_FIRST for dc in (0, 1) if (dz, dy, dc) != (0, 0, 0)
    ]

    def split_taps():
        for jb in range(J // 8):
            t = [taps[pl.ds(jb * 64 + ((k // 8) * 256 + k % 8), 8, stride=8), :] for k in range(TAPS)]
            for i in range(quarter):
                a, b, c, d = t[4 * i:4 * i + 4]
                for place, h in enumerate((a, c, a + c, b, d, b + d, a + b, c + d, (a + b) + (c + d))):
                    tap_sums[jb, place, i] = h

    def fir(first, count, s, jb, slot):
        groups_of_four = count // 4
        keep = xbuf.at[jb % 2]

        def sample(g):
            return vbuf.at[s, (first + g + 16) // 8][pl.ds(jb * 64 + (g + 16) % 8, 8, stride=8), :]

        def run(h, x):
            total = h[0] * x[quarter - 1]
            for i in range(1, quarter):
                total = total + h[i] * x[quarter - 1 - i]
            return total

        def nested(level, even, odd, give):
            h = [[tap_sums[jb, 3 * level + k, i] for i in range(quarter)] for k in range(3)]
            x = [even(n) for n in range(1 - quarter, 0)]
            y = [odd(n) for n in range(-quarter, 0)]
            z = [a + b for a, b in zip(x, y[1:])]
            before = run(h[1], y)
            for n in range(groups_of_four):
                x, y = x[1 - quarter:] + [even(n)], y[1:] + [odd(n)]
                z = z[1 - quarter:] + [x[-1] + y[-1]]
                a, b, ab = run(h[0], x), run(h[1], y), run(h[2], z)
                give(n, a + before, ab - (a + b))
                before = b

        place = pl.ds(s * J + jb * 8, 8)
        def even_samples(n, h):
            value = sample(4 * n + 2 * h)
            keep[0, 2 * n + h + 2 * quarter] = value
            return value

        def odd_samples(n, h):
            value = sample(4 * n + 2 * h + 1)
            keep[1, 2 * n + h + 2 * quarter] = value + keep[0, 2 * n + h + 2 * quarter]
            return value

        def sums(n, h):
            return keep[1, 2 * n + h + 2 * quarter]

        def give_even(n, u, v):
            keep[2, 2 * n], keep[2, 2 * n + 1] = u, v

        carried = []

        def give_odd(n, u, v):
            a, b = keep[2, 2 * n], keep[2, 2 * n + 1]
            ybuf[slot, 4 * n, place, :] = a + carried[-1]
            ybuf[slot, 4 * n + 2, place, :] = b + u
            keep[3, 2 * n], keep[3, 2 * n + 1] = a + u, b + v
            carried.append(v)

        def give_sum(n, u, v):
            ybuf[slot, 4 * n + 1, place, :] = u - keep[3, 2 * n]
            ybuf[slot, 4 * n + 3, place, :] = v - keep[3, 2 * n + 1]

        def start():
            total = None
            for i in range(quarter):
                for k in range(2):
                    term = tap_sums[jb, 3 + k, i] * sample(-1 - 4 * i - 2 * k)
                    total = term if total is None else total + term
            carried.append(total)

        start()
        nested(0, lambda n: even_samples(n, 0), lambda n: even_samples(n, 1), give_even)
        nested(1, lambda n: odd_samples(n, 0), lambda n: odd_samples(n, 1), give_odd)
        nested(2, lambda n: sums(n, 0), lambda n: sums(n, 1), give_sum)

    def first_stage(part, slot):
        cosine, sine = twist[0], twist[1]
        for pair in range(4):
            f = part * 8 + pair * 2
            y = jnp.concatenate([ybuf[slot, f], ybuf[slot, f + 1]], axis=1)
            high, low = split(y)
            o = dot(outer[...], jnp.concatenate([high, low, high], axis=0))
            for h in range(2):
                re, im = o[:J, h * L:(h + 1) * L], o[J:, h * L:(h + 1) * L]
                z = jnp.concatenate([re * cosine + im * sine, im * cosine - re * sine], axis=1)
                place = pl.ds((pair * 2 + h) * J, J)
                zbuf[part, 0, place, :], zbuf[part, 1, place, :] = split(z)

    def second_stage(part, slot):
        high, low = zbuf[part, 0], zbuf[part, 1]
        x = dot(high, inner[0]) + dot(low, inner[0]) + dot(high, inner[1])
        power = x[:, :L] * x[:, :L] + x[:, L:] * x[:, L:]
        for r in range(2):
            p = [power[(4 * r + f) * J:(4 * r + f + 1) * J] for f in range(4)]
            row = (p[0] + p[1]) + (p[2] + p[3])
            moments[0] += row
            moments[1] += (p[0] * p[0] + p[1] * p[1]) + (p[2] * p[2] + p[3] * p[3])
            held[slot, part * 2 + r] = row

    def clean_lanes():
        block = lax.broadcasted_iota(jnp.int32, (groups, L), 0)
        lane = lax.broadcasted_iota(jnp.int32, (groups, L), 1)
        spread_out = jnp.where(lane // 4 == block, 1.0, 0.0)
        clean = jnp.broadcast_to(1.0 - flags[...].astype(F32), (8, groups))
        return dot(clean.astype(BF16), spread_out.astype(BF16))[0:1]

    def finish_rows(slot, side, target):
        clean = moments[2, pl.ds(8, 1), :]
        lane = lax.broadcasted_iota(jnp.int32, (1, L), 1)
        rows, inverse, summed = [], None, None
        for a in range(4):
            row = held[slot, side * 4 + a]
            part = jnp.sum(row, axis=0, keepdims=True) * clean
            one = jnp.broadcast_to(1.0 / jnp.sum(part, axis=1, keepdims=True), (1, L))
            inverse = one if a == 0 else jnp.where(lane % 4 == a, one, inverse)
            summed = part if a == 0 else summed + part
            rows.append(row * float(J * L))
        moments[2, pl.ds(0, 1), :] += summed
        target[...] = owners_first(rows, clean * inverse).reshape(groups, 4, L)

    def in_turn(one, count):
        def some(dests):
            for dest in dests:
                one(dest).start()

        return [functools.partial(some, others[n::count]) for n in range(count)]

    def send_wide(g):
        return in_turn(
            lambda dest: send(wide.at[g, dest], dyn.at[me, pl.ds(1 + 2 * g, 2)], dest, row_send, row_recv), 8
        )

    def send_late():
        return in_turn(lambda dest: send(late.at[dest], dyn.at[me, pl.ds(5, 3)], dest, row_send, row_recv), 8)

    pieces = [(s, jb) for s in range(2) for jb in range(J // 8)]

    def stages(parts, slot):
        order = [functools.partial(first_stage, 0, slot)]
        for part in range(1, parts):
            order.append(functools.partial(first_stage, part, slot))
            order.append(functools.partial(second_stage, part - 1, slot))
        return order + [functools.partial(second_stage, parts - 1, slot)]

    def interleave(*lists):
        keyed = [((n + 0.5) / len(one), k, action) for k, one in enumerate(lists) for n, action in enumerate(one)]
        for _, _, action in sorted(keyed, key=lambda entry: entry[:2]):
            action()

    def filters(first, count, slot):
        return [functools.partial(fir, first, count, s, jb, slot) for s, jb in pieces]

    moments[...] = jnp.zeros_like(moments)

    loads[0].wait()
    split_taps()
    loads[1].wait()
    near_entered()

    @pl.when(me < groups - 1)
    def _():
        halo(0).start()
        halo(1).start()

    for dest in across:
        signal(ready, dest)
    loads[2].wait()
    for action in filters(16, 32, 0)[:4]:
        action()
    loads[3].wait()
    for action in filters(16, 32, 0)[4:]:
        action()
    for piece in range(4, 10):
        loads[piece].wait()
    moments[2, pl.ds(8, 1), :] = clean_lanes()

    def finish(slot, side, target):
        return functools.partial(finish_rows, slot, side, target)

    interleave(filters(48, 32, 1))
    interleave(stages(4, 0))
    interleave(stages(4, 1), [finish(0, side, wide.at[0, :, side]) for side in range(2)])
    interleave(filters(80, 32, 0)[:2])
    pl.semaphore_wait(ready, 3)
    interleave(filters(80, 32, 0)[2:], [finish(1, side, wide.at[1, :, side]) for side in range(2)], send_wide(0))
    interleave(filters(112, 16, 1), send_wide(1))
    interleave(stages(4, 0))
    interleave(stages(2, 1), [finish(0, side, late.at[:, side]) for side in range(2)])
    finish_rows(1, 0, late.at[:, 2])

    for s in range(2):
        @pl.when(me > 0)
        def _():
            halo(s).wait_recv()

        @pl.when(me == 0)
        def _():
            vbuf[s, pl.ds(0, 2)] = jnp.zeros((2, 8 * J, L), F32)

        interleave(filters(0, 16, 0)[4 * s:4 * s + 4], [] if s else send_late())
    interleave(stages(2, 0))
    finish_rows(0, 0, final.at[:, 0])

    local = jnp.sum(moments[2, pl.ds(0, 1), :], axis=1, keepdims=True)
    last = [moments[0], moments[1], jnp.broadcast_to(local, (J, L)), jnp.zeros((J, L), F32)]
    final[:, 1] = owners_first(last).reshape(groups, 4, L)
    for dest in others:
        send(final.at[dest], got.at[me], dest, fin_send, fin_recv).start()
    got[me] = final[me]
    for g in range(2):
        dyn[me, pl.ds(1 + 2 * g, 2)] = wide[g, me]
    dyn[me, pl.ds(5, 3)] = late[me]

    everyone = pl.ds(0, groups - 1)
    send(final.at[everyone], got.at[everyone], following, fin_send, fin_recv).wait_recv()
    lane = lax.broadcasted_iota(jnp.int32, (1, L), 1)
    own = jnp.sum(jnp.where(lane == 4 * me, moments[2, pl.ds(8, 1), :], 0.0), axis=1, keepdims=True)
    mine[...] = jnp.broadcast_to(own, (1, L))

    units = dyn.at[everyone, pl.ds(1, 7)]
    send(units, units, following, row_send, row_recv).wait()
    send(final.at[everyone], got.at[everyone], following, fin_send, fin_recv).wait_send()

    @pl.when(me < groups - 1)
    def _():
        halo(0).wait_send()
        halo(1).wait_send()


def deliver(count, dyn, got, mine, rows, kurt, spec, kbuf, sbuf, sem):
    later = pltpu.make_async_copy(dyn.at[:, pl.ds(1, 7)], rows.at[:, pl.ds(1, 7)], sem.at[0])
    early = pltpu.make_async_copy(got.at[:, 0], rows.at[:, 0], sem.at[1])
    later.start()
    early.start()
    sums = jnp.sum(got[:, 1], axis=0)
    first, second, group = sums[0:1], sums[1:2], sums[2:3]
    kbuf[...] = (count + 1.0) / (count - 1.0) * (count * second / (first * first) - 1.0)
    sbuf[...] = float(J * L) * mine[...] * first / group
    small = [pltpu.make_async_copy(kbuf, kurt, sem.at[2]), pltpu.make_async_copy(sbuf, spec, sem.at[3])]
    for one in small:
        one.start()
    for one in small:
        one.wait()
    later.wait()
    early.wait()


def body(groups, voltages, taps, flags):
    frames = voltages.shape[1]
    volt = voltages.reshape(2, frames // 8, 8, J, L).transpose(0, 1, 3, 2, 4).reshape(2, frames // 8, 8 * J, L)
    tap = taps.reshape(TAPS // 8, 8, J, L).transpose(0, 2, 1, 3).reshape(TAPS * J, L)
    outer, twist, inner = tables()
    vmem = pl.BlockSpec(memory_space=pltpu.VMEM)
    operands = (volt, tap, flags.reshape(1, groups), jnp.asarray(outer), jnp.asarray(twist), jnp.asarray(inner))
    received = pl.pallas_call(
        functools.partial(kernel, groups, frames),
        out_shape=(
            jax.ShapeDtypeStruct((groups, frames // 16, 4, L), F32),
            jax.ShapeDtypeStruct((groups, 2, 4, L), F32),
            jax.ShapeDtypeStruct((1, L), F32),
        ),
        in_specs=[pl.BlockSpec(memory_space=pltpu.HBM)] * 6,
        out_specs=(vmem, vmem, vmem),
        scratch_shapes=[
            pltpu.VMEM((2, frames // 8 + 2, 8 * J, L), F32),
            pltpu.VMEM((TAPS * J, L), F32),
            pltpu.VMEM((1, groups), jnp.int32),
            pltpu.VMEM(outer.shape, BF16),
            pltpu.VMEM(twist.shape, F32),
            pltpu.VMEM(inner.shape, BF16),
            pltpu.VMEM((J // 8, 9, TAPS // 4, 8, L), F32),
            pltpu.VMEM((2, 4, CHUNK // 2 + TAPS // 2, 8, L), F32),
            pltpu.VMEM((2, CHUNK, 2 * J, L), F32),
            pltpu.VMEM((CHUNK // 8, 2, 8 * J, 2 * L), BF16),
            pltpu.VMEM((2, CHUNK // 4, J, L), F32),
            pltpu.VMEM((2, groups, 2, 4, L), F32),
            pltpu.VMEM((groups, 3, 4, L), F32),
            pltpu.VMEM((groups, 2, 4, L), F32),
            pltpu.VMEM((3, J, L), F32),
            pltpu.SemaphoreType.DMA((10,)),
            pltpu.SemaphoreType.REGULAR,
            pltpu.SemaphoreType.DMA((2,)),
            pltpu.SemaphoreType.DMA((2,)),
        ] + [pltpu.SemaphoreType.DMA] * 4,
        compiler_params=pltpu.CompilerParams(
            collective_id=0, has_side_effects=True, vmem_limit_bytes=40 * 1024 * 1024
        ),
    )(*(pltpu.with_memory_space_constraint(x, pltpu.HBM) for x in operands))
    hbm = pl.BlockSpec(memory_space=pltpu.HBM)
    dyn, kurt, spec = pl.pallas_call(
        functools.partial(deliver, float(frames * groups)),
        out_shape=(
            jax.ShapeDtypeStruct((groups, frames // 16, 4, L), F32),
            jax.ShapeDtypeStruct((1, L), F32),
            jax.ShapeDtypeStruct((1, L), F32),
        ),
        in_specs=[vmem] * 3,
        out_specs=(hbm, hbm, hbm),
        scratch_shapes=[pltpu.VMEM((1, L), F32), pltpu.VMEM((1, L), F32), pltpu.SemaphoreType.DMA((4,))],
        compiler_params=pltpu.CompilerParams(vmem_limit_bytes=4 * 1024 * 1024),
    )(*received)
    return dyn.reshape(groups * frames // 4, L), kurt.reshape(L), spec.reshape(L)


def solution(mesh):
    placed = (P(None, ("stream", "tm"), None), P(), P("stream"))
    return jax.shard_map(
        functools.partial(body, mesh.shape["tm"]),
        mesh=mesh,
        in_specs=placed,
        out_specs=(P("stream", "tm"), P(("stream", "tm")), P(("stream", "tm"))),
        check_vma=False,
    )
```

```python
import functools

import jax
import jax.numpy as jnp
import ml_dtypes
import numpy as np
from jax import lax
from jax.experimental import pallas as pl
from jax.experimental.pallas import tpu as pltpu
from jax.sharding import PartitionSpec as P

J, L = 32, 128
TAPS = 16
CHUNK = 32
FAR_FIRST = sorted(
    ((dz, dy) for dz in range(4) for dy in range(4)), key=lambda d: -(min(d[0], 4 - d[0]) + min(d[1], 4 - d[1]))
)
F32, BF16 = jnp.float32, jnp.bfloat16
MESH = pl.DeviceIdType.MESH


def split_table(table):
    high = table.astype(ml_dtypes.bfloat16)
    low = (table - high.astype(np.float64)).astype(ml_dtypes.bfloat16)
    return high, low


def complex_table(turns, steps):
    angle = 2.0 * np.pi * (turns % steps) / steps
    cosine, sine = np.cos(angle), np.sin(angle)
    return cosine, sine


def tables():
    q, j = np.arange(J)[:, None], np.arange(J)[None, :]
    cosine, sine = complex_table(q * j, J)
    outer = np.block([[cosine, sine], [-sine, cosine]])
    high, low = split_table(outer)
    outer_table = np.concatenate([high, high, low], 1)
    cosine, sine = complex_table(q * np.arange(L)[None, :], J * L)
    twist = np.stack([cosine, sine]).astype(np.float32)
    a, m = np.arange(L)[:, None], np.arange(L)[None, :]
    cosine, sine = complex_table(a * m, L)
    inner = np.block([[cosine, -sine], [sine, cosine]])
    return outer_table, twist, np.stack(split_table(inner))


def split(value):
    high = value.astype(BF16)
    low = (value - high.astype(F32)).astype(BF16)
    return high, low


def dot(a, b):
    return jnp.dot(a, b, preferred_element_type=F32)


def exchange(rows):
    lane = lax.broadcasted_iota(jnp.int32, rows[0].shape, 1)
    rows = list(rows)
    for bit in (2, 1):
        upper = (lane & bit) != 0
        for a in range(4):
            if a & bit:
                continue
            x, y = rows[a], rows[a + bit]
            rows[a] = jnp.where(upper, pltpu.roll(y, bit, 1), x)
            rows[a + bit] = jnp.where(upper, y, pltpu.roll(x, L - bit, 1))
    return rows


def owners_first(rows, scale=None):
    rows = exchange(rows)
    if scale is not None:
        rows = [row * scale for row in rows]
    return jnp.concatenate(rows, axis=0).T


def kernel(
    groups, frames,
    volt, taps_in, flags_in, outer_in, twist_in, inner_in,
    dyn, got, mine,
    vbuf, taps, flags, outer, twist, inner, tap_sums, xbuf, ybuf, zbuf, held, wide, late, final, moments,
    load_sem, ready, halo_send, halo_recv, row_send, row_recv, fin_send, fin_recv,
):
    me = lax.axis_index("tm")
    blocks = frames // 8
    quarter = TAPS // 4
    both = pl.ds(0, 2)
    following = lax.rem(me + 1, groups)

    def load(piece, part, first, count):
        return pltpu.make_async_copy(
            volt.at[part, pl.ds(first, count)], vbuf.at[part, pl.ds(first + 2, count)], load_sem.at[piece]
        )

    loads = [
        pltpu.make_async_copy(taps_in, taps, load_sem.at[0]),
        load(1, both, blocks - 2, 2),
        load(2, 0, 0, 6),
        load(3, 1, 0, 6),
        pltpu.make_async_copy(outer_in, outer, load_sem.at[4]),
        pltpu.make_async_copy(twist_in, twist, load_sem.at[5]),
        pltpu.make_async_copy(inner_in, inner, load_sem.at[6]),
        pltpu.make_async_copy(flags_in, flags, load_sem.at[7]),
        load(8, both, 6, 4),
        load(9, both, 10, 4),
    ]
    def signal(semaphore, dest):
        pl.semaphore_signal(semaphore, 1, device_id={"tm": dest}, device_id_type=MESH)

    barrier = pltpu.get_barrier_semaphore()
    column, core, plane = me // 2 % 4, me % 2, me // 8
    line = [plane * 8 + lax.rem(me + d, 8) for d in (1, 7, 2, 6, 3, 5, 4)]
    across = [lax.rem(me + 8 * d, groups) for d in range(1, 4)]
    for dest in line + across:
        signal(barrier, dest)
    ends = (lax.rem(me, 8) == 7, lax.rem(me, 8) == 0)

    @pl.when(ends[0])
    def _():
        signal(barrier, following)

    @pl.when(ends[1])
    def _():
        signal(barrier, lax.rem(me + groups - 1, groups))

    for one in loads:
        one.start()

    def near_entered():
        place = lax.rem(me, 8)
        pl.semaphore_wait(barrier, 10 + lax.div(place, 7) + lax.div(7 - place, 7))

    def send(src, dst, dest, send_sem, recv_sem):
        return pltpu.make_async_remote_copy(
            src, dst, send_sem, recv_sem, device_id={"tm": dest}, device_id_type=MESH
        )

    def halo(part):
        s, rows = part // 2, pl.ds(part % 2 * 4 * J, 4 * J)
        return send(
            vbuf.at[s, pl.ds(blocks, 2), rows], vbuf.at[s, pl.ds(0, 2), rows],
            following, halo_send.at[part], halo_recv.at[part],
        )

    others = [
        lax.rem(plane + dz, 4) * 8 + lax.rem(column + dy, 4) * 2 + lax.rem(core + dc, 2)
        for dz, dy in FAR_FIRST for dc in (0, 1) if (dz, dy, dc) != (0, 0, 0)
    ]

    def split_taps():
        for jb in range(J // 8):
            t = [taps[pl.ds(jb * 64 + ((k // 8) * 256 + k % 8), 8, stride=8), :] for k in range(TAPS)]
            for i in range(quarter):
                a, b, c, d = t[4 * i:4 * i + 4]
                for place, h in enumerate((a, c, a + c, b, d, b + d, a + b, c + d, (a + b) + (c + d))):
                    tap_sums[jb, place, i] = h

    def fir(first, count, s, jb, slot):
        groups_of_four = count // 4
        keep = xbuf.at[jb % 2]

        def sample(g):
            return vbuf.at[s, (first + g + 16) // 8][pl.ds(jb * 64 + (g + 16) % 8, 8, stride=8), :]

        def run(h, x):
            total = h[0] * x[quarter - 1]
            for i in range(1, quarter):
                total = total + h[i] * x[quarter - 1 - i]
            return total

        def nested(level, even, odd, give):
            h = [[tap_sums[jb, 3 * level + k, i] for i in range(quarter)] for k in range(3)]
            x = [even(n) for n in range(1 - quarter, 0)]
            y = [odd(n) for n in range(-quarter, 0)]
            z = [a + b for a, b in zip(x, y[1:])]
            before = run(h[1], y)
            for n in range(groups_of_four):
                x, y = x[1 - quarter:] + [even(n)], y[1:] + [odd(n)]
                z = z[1 - quarter:] + [x[-1] + y[-1]]
                a, b, ab = run(h[0], x), run(h[1], y), run(h[2], z)
                give(n, a + before, ab - (a + b))
                before = b

        place = pl.ds(s * J + jb * 8, 8)
        def even_samples(n, h):
            value = sample(4 * n + 2 * h)
            keep[0, 2 * n + h + 2 * quarter] = value
            return value

        def odd_samples(n, h):
            value = sample(4 * n + 2 * h + 1)
            keep[1, 2 * n + h + 2 * quarter] = value + keep[0, 2 * n + h + 2 * quarter]
            return value

        def sums(n, h):
            return keep[1, 2 * n + h + 2 * quarter]

        def give_even(n, u, v):
            keep[2, 2 * n], keep[2, 2 * n + 1] = u, v

        carried = []

        def give_odd(n, u, v):
            a, b = keep[2, 2 * n], keep[2, 2 * n + 1]
            ybuf[slot, 4 * n, place, :] = a + carried[-1]
            ybuf[slot, 4 * n + 2, place, :] = b + u
            keep[3, 2 * n], keep[3, 2 * n + 1] = a + u, b + v
            carried.append(v)

        def give_sum(n, u, v):
            ybuf[slot, 4 * n + 1, place, :] = u - keep[3, 2 * n]
            ybuf[slot, 4 * n + 3, place, :] = v - keep[3, 2 * n + 1]

        def start():
            total = None
            for i in range(quarter):
                for k in range(2):
                    term = tap_sums[jb, 3 + k, i] * sample(-1 - 4 * i - 2 * k)
                    total = term if total is None else total + term
            carried.append(total)

        start()
        nested(0, lambda n: even_samples(n, 0), lambda n: even_samples(n, 1), give_even)
        nested(1, lambda n: odd_samples(n, 0), lambda n: odd_samples(n, 1), give_odd)
        nested(2, lambda n: sums(n, 0), lambda n: sums(n, 1), give_sum)

    def first_stage(part, slot):
        cosine, sine = twist[0], twist[1]
        for pair in range(4):
            f = part * 8 + pair * 2
            y = jnp.concatenate([ybuf[slot, f], ybuf[slot, f + 1]], axis=1)
            high, low = split(y)
            o = dot(outer[...], jnp.concatenate([high, low, high], axis=0))
            for h in range(2):
                re, im = o[:J, h * L:(h + 1) * L], o[J:, h * L:(h + 1) * L]
                z = jnp.concatenate([re * cosine + im * sine, im * cosine - re * sine], axis=1)
                place = pl.ds((pair * 2 + h) * J, J)
                zbuf[part, 0, place, :], zbuf[part, 1, place, :] = split(z)

    def second_stage(part, slot):
        high, low = zbuf[part, 0], zbuf[part, 1]
        x = dot(high, inner[0]) + dot(low, inner[0]) + dot(high, inner[1])
        power = x[:, :L] * x[:, :L] + x[:, L:] * x[:, L:]
        for r in range(2):
            p = [power[(4 * r + f) * J:(4 * r + f + 1) * J] for f in range(4)]
            row = (p[0] + p[1]) + (p[2] + p[3])
            moments[0] += row
            moments[1] += (p[0] * p[0] + p[1] * p[1]) + (p[2] * p[2] + p[3] * p[3])
            held[slot, part * 2 + r] = row

    def clean_lanes():
        block = lax.broadcasted_iota(jnp.int32, (groups, L), 0)
        lane = lax.broadcasted_iota(jnp.int32, (groups, L), 1)
        spread_out = jnp.where(lane // 4 == block, 1.0, 0.0)
        clean = jnp.broadcast_to(1.0 - flags[...].astype(F32), (8, groups))
        return dot(clean.astype(BF16), spread_out.astype(BF16))[0:1]

    def finish_rows(slot, side, target):
        clean = moments[2, pl.ds(8, 1), :]
        lane = lax.broadcasted_iota(jnp.int32, (1, L), 1)
        rows, inverse, summed = [], None, None
        for a in range(4):
            row = held[slot, side * 4 + a]
            part = jnp.sum(row, axis=0, keepdims=True) * clean
            one = jnp.broadcast_to(1.0 / jnp.sum(part, axis=1, keepdims=True), (1, L))
            inverse = one if a == 0 else jnp.where(lane % 4 == a, one, inverse)
            summed = part if a == 0 else summed + part
            rows.append(row * float(J * L))
        moments[2, pl.ds(0, 1), :] += summed
        target[...] = owners_first(rows, clean * inverse).reshape(groups, 4, L)

    def in_turn(one, count):
        def some(dests):
            for dest in dests:
                one(dest).start()

        return [functools.partial(some, others[n::count]) for n in range(count)]

    def send_wide(g):
        return in_turn(
            lambda dest: send(wide.at[g, dest], dyn.at[me, pl.ds(1 + 2 * g, 2)], dest, row_send, row_recv), 8
        )

    def send_late():
        return in_turn(lambda dest: send(late.at[dest], dyn.at[me, pl.ds(5, 3)], dest, row_send, row_recv), 8)

    pieces = [(s, jb) for s in range(2) for jb in range(J // 8)]

    def stages(parts, slot):
        order = [functools.partial(first_stage, 0, slot)]
        for part in range(1, parts):
            order.append(functools.partial(first_stage, part, slot))
            order.append(functools.partial(second_stage, part - 1, slot))
        return order + [functools.partial(second_stage, parts - 1, slot)]

    def interleave(*lists):
        keyed = [((n + 0.5) / len(one), k, action) for k, one in enumerate(lists) for n, action in enumerate(one)]
        for _, _, action in sorted(keyed, key=lambda entry: entry[:2]):
            action()

    def filters(first, count, slot):
        return [functools.partial(fir, first, count, s, jb, slot) for s, jb in pieces]

    moments[...] = jnp.zeros_like(moments)

    loads[0].wait()
    split_taps()
    loads[1].wait()
    near_entered()

    @pl.when(me < groups - 1)
    def _():
        for part in range(4):
            halo(part).start()

    for dest in across:
        signal(ready, dest)
    loads[2].wait()
    for action in filters(16, 32, 0)[:4]:
        action()
    loads[3].wait()
    for action in filters(16, 32, 0)[4:]:
        action()
    for piece in range(4, 10):
        loads[piece].wait()
    moments[2, pl.ds(8, 1), :] = clean_lanes()

    def finish(slot, side, target):
        return functools.partial(finish_rows, slot, side, target)

    interleave(filters(48, 32, 1))
    interleave(stages(4, 0))
    interleave(stages(4, 1), [finish(0, side, wide.at[0, :, side]) for side in range(2)])
    interleave(filters(80, 32, 0)[:2])
    pl.semaphore_wait(ready, 3)
    interleave(filters(80, 32, 0)[2:], [finish(1, side, wide.at[1, :, side]) for side in range(2)], send_wide(0))
    interleave(filters(112, 16, 1), send_wide(1))
    interleave(stages(4, 0))
    interleave(stages(2, 1), [finish(0, side, late.at[:, side]) for side in range(2)])
    finish_rows(1, 0, late.at[:, 2])

    @pl.when(me == 0)
    def _():
        vbuf[:, pl.ds(0, 2)] = jnp.zeros((2, 2, 8 * J, L), F32)

    for part in range(4):
        @pl.when(me > 0)
        def _():
            halo(part).wait_recv()

        interleave(filters(0, 16, 0)[2 * part:2 * part + 2], send_late()[4 * part:4 * part + 4])

    interleave(stages(2, 0))
    finish_rows(0, 0, final.at[:, 0])

    local = jnp.sum(moments[2, pl.ds(0, 1), :], axis=1, keepdims=True)
    last = [moments[0], moments[1], jnp.broadcast_to(local, (J, L)), jnp.zeros((J, L), F32)]
    final[:, 1] = owners_first(last).reshape(groups, 4, L)
    for dest in others:
        send(final.at[dest], got.at[me], dest, fin_send, fin_recv).start()
    got[me] = final[me]
    for g in range(2):
        dyn[me, pl.ds(1 + 2 * g, 2)] = wide[g, me]
    dyn[me, pl.ds(5, 3)] = late[me]

    everyone = pl.ds(0, groups - 1)
    send(final.at[everyone], got.at[everyone], following, fin_send, fin_recv).wait_recv()
    lane = lax.broadcasted_iota(jnp.int32, (1, L), 1)
    own = jnp.sum(jnp.where(lane == 4 * me, moments[2, pl.ds(8, 1), :], 0.0), axis=1, keepdims=True)
    mine[...] = jnp.broadcast_to(own, (1, L))

    units = dyn.at[everyone, pl.ds(1, 7)]
    send(units, units, following, row_send, row_recv).wait()
    send(final.at[everyone], got.at[everyone], following, fin_send, fin_recv).wait_send()

    @pl.when(me < groups - 1)
    def _():
        for part in range(4):
            halo(part).wait_send()


def deliver(count, dyn, got, mine, rows, kurt, spec, kbuf, sbuf, sem):
    later = pltpu.make_async_copy(dyn.at[:, pl.ds(1, 7)], rows.at[:, pl.ds(1, 7)], sem.at[0])
    early = pltpu.make_async_copy(got.at[:, 0], rows.at[:, 0], sem.at[1])
    later.start()
    early.start()
    sums = jnp.sum(got[:, 1], axis=0)
    first, second, group = sums[0:1], sums[1:2], sums[2:3]
    kbuf[...] = (count + 1.0) / (count - 1.0) * (count * second / (first * first) - 1.0)
    sbuf[...] = float(J * L) * mine[...] * first / group
    small = [pltpu.make_async_copy(kbuf, kurt, sem.at[2]), pltpu.make_async_copy(sbuf, spec, sem.at[3])]
    for one in small:
        one.start()
    for one in small:
        one.wait()
    later.wait()
    early.wait()


def body(groups, voltages, taps, flags):
    frames = voltages.shape[1]
    volt = voltages.reshape(2, frames // 8, 8, J, L).transpose(0, 1, 3, 2, 4).reshape(2, frames // 8, 8 * J, L)
    tap = taps.reshape(TAPS // 8, 8, J, L).transpose(0, 2, 1, 3).reshape(TAPS * J, L)
    outer, twist, inner = tables()
    vmem = pl.BlockSpec(memory_space=pltpu.VMEM)
    operands = (volt, tap, flags.reshape(1, groups), jnp.asarray(outer), jnp.asarray(twist), jnp.asarray(inner))
    received = pl.pallas_call(
        functools.partial(kernel, groups, frames),
        out_shape=(
            jax.ShapeDtypeStruct((groups, frames // 16, 4, L), F32),
            jax.ShapeDtypeStruct((groups, 2, 4, L), F32),
            jax.ShapeDtypeStruct((1, L), F32),
        ),
        in_specs=[pl.BlockSpec(memory_space=pltpu.HBM)] * 6,
        out_specs=(vmem, vmem, vmem),
        scratch_shapes=[
            pltpu.VMEM((2, frames // 8 + 2, 8 * J, L), F32),
            pltpu.VMEM((TAPS * J, L), F32),
            pltpu.VMEM((1, groups), jnp.int32),
            pltpu.VMEM(outer.shape, BF16),
            pltpu.VMEM(twist.shape, F32),
            pltpu.VMEM(inner.shape, BF16),
            pltpu.VMEM((J // 8, 9, TAPS // 4, 8, L), F32),
            pltpu.VMEM((2, 4, CHUNK // 2 + TAPS // 2, 8, L), F32),
            pltpu.VMEM((2, CHUNK, 2 * J, L), F32),
            pltpu.VMEM((CHUNK // 8, 2, 8 * J, 2 * L), BF16),
            pltpu.VMEM((2, CHUNK // 4, J, L), F32),
            pltpu.VMEM((2, groups, 2, 4, L), F32),
            pltpu.VMEM((groups, 3, 4, L), F32),
            pltpu.VMEM((groups, 2, 4, L), F32),
            pltpu.VMEM((3, J, L), F32),
            pltpu.SemaphoreType.DMA((10,)),
            pltpu.SemaphoreType.REGULAR,
            pltpu.SemaphoreType.DMA((4,)),
            pltpu.SemaphoreType.DMA((4,)),
        ] + [pltpu.SemaphoreType.DMA] * 4,
        compiler_params=pltpu.CompilerParams(
            collective_id=0, has_side_effects=True, vmem_limit_bytes=40 * 1024 * 1024
        ),
    )(*(pltpu.with_memory_space_constraint(x, pltpu.HBM) for x in operands))
    hbm = pl.BlockSpec(memory_space=pltpu.HBM)
    dyn, kurt, spec = pl.pallas_call(
        functools.partial(deliver, float(frames * groups)),
        out_shape=(
            jax.ShapeDtypeStruct((groups, frames // 16, 4, L), F32),
            jax.ShapeDtypeStruct((1, L), F32),
            jax.ShapeDtypeStruct((1, L), F32),
        ),
        in_specs=[vmem] * 3,
        out_specs=(hbm, hbm, hbm),
        scratch_shapes=[pltpu.VMEM((1, L), F32), pltpu.VMEM((1, L), F32), pltpu.SemaphoreType.DMA((4,))],
        compiler_params=pltpu.CompilerParams(vmem_limit_bytes=4 * 1024 * 1024),
    )(*received)
    return dyn.reshape(groups * frames // 4, L), kurt.reshape(L), spec.reshape(L)


def solution(mesh):
    placed = (P(None, ("stream", "tm"), None), P(), P("stream"))
    return jax.shard_map(
        functools.partial(body, mesh.shape["tm"]),
        mesh=mesh,
        in_specs=placed,
        out_specs=(P("stream", "tm"), P(("stream", "tm")), P(("stream", "tm"))),
        check_vma=False,
    )
```

```python
import functools

import jax
import jax.numpy as jnp
import ml_dtypes
import numpy as np
from jax import lax
from jax.experimental import pallas as pl
from jax.experimental.pallas import tpu as pltpu
from jax.sharding import PartitionSpec as P

J, L = 32, 128
TAPS = 16
CHUNK = 32
FAR_FIRST = sorted(
    ((dz, dy) for dz in range(4) for dy in range(4)), key=lambda d: -(min(d[0], 4 - d[0]) + min(d[1], 4 - d[1]))
)
F32, BF16 = jnp.float32, jnp.bfloat16
MESH = pl.DeviceIdType.MESH


def split_table(table):
    high = table.astype(ml_dtypes.bfloat16)
    low = (table - high.astype(np.float64)).astype(ml_dtypes.bfloat16)
    return high, low


def complex_table(turns, steps):
    angle = 2.0 * np.pi * (turns % steps) / steps
    cosine, sine = np.cos(angle), np.sin(angle)
    return cosine, sine


def tables():
    q, j = np.arange(J)[:, None], np.arange(J)[None, :]
    cosine, sine = complex_table(q * j, J)
    outer = np.block([[cosine, sine], [-sine, cosine]])
    high, low = split_table(outer)
    outer_table = np.concatenate([high, high, low], 1)
    cosine, sine = complex_table(q * np.arange(L)[None, :], J * L)
    twist = np.stack([cosine, sine]).astype(np.float32)
    a, m = np.arange(L)[:, None], np.arange(L)[None, :]
    cosine, sine = complex_table(a * m, L)
    inner = np.block([[cosine, -sine], [sine, cosine]])
    return outer_table, twist, np.stack(split_table(inner))


def split(value):
    high = value.astype(BF16)
    low = (value - high.astype(F32)).astype(BF16)
    return high, low


def dot(a, b):
    return jnp.dot(a, b, preferred_element_type=F32)


def exchange(rows):
    lane = lax.broadcasted_iota(jnp.int32, rows[0].shape, 1)
    rows = list(rows)
    for bit in (2, 1):
        upper = (lane & bit) != 0
        for a in range(4):
            if a & bit:
                continue
            x, y = rows[a], rows[a + bit]
            rows[a] = jnp.where(upper, pltpu.roll(y, bit, 1), x)
            rows[a + bit] = jnp.where(upper, y, pltpu.roll(x, L - bit, 1))
    return rows


def owners_first(rows, scale=None):
    rows = exchange(rows)
    if scale is not None:
        rows = [row * scale for row in rows]
    return jnp.concatenate(rows, axis=0).T


def kernel(
    groups, frames,
    volt, taps_in, flags_in, outer_in, twist_in, inner_in,
    dyn, got, mine,
    vbuf, taps, flags, outer, twist, inner, tap_sums, xbuf, ybuf, zbuf, held, wide, late, final, moments,
    load_sem, ready, halo_send, halo_recv, row_send, row_recv, fin_send, fin_recv,
):
    me = lax.axis_index("tm")
    blocks = frames // 8
    quarter = TAPS // 4
    both = pl.ds(0, 2)
    following = lax.rem(me + 1, groups)

    def load(piece, part, first, count):
        return pltpu.make_async_copy(
            volt.at[part, pl.ds(first, count)], vbuf.at[part, pl.ds(first + 2, count)], load_sem.at[piece]
        )

    loads = [
        pltpu.make_async_copy(taps_in, taps, load_sem.at[0]),
        load(1, both, blocks - 2, 2),
        load(2, 0, 0, 6),
        load(3, 1, 0, 6),
        pltpu.make_async_copy(outer_in, outer, load_sem.at[4]),
        pltpu.make_async_copy(twist_in, twist, load_sem.at[5]),
        pltpu.make_async_copy(inner_in, inner, load_sem.at[6]),
        pltpu.make_async_copy(flags_in, flags, load_sem.at[7]),
        load(8, both, 6, 4),
        load(9, both, 10, 4),
    ]
    def signal(semaphore, dest):
        pl.semaphore_signal(semaphore, 1, device_id={"tm": dest}, device_id_type=MESH)

    barrier = pltpu.get_barrier_semaphore()
    column, core, plane = me // 2 % 4, me % 2, me // 8
    line = [plane * 8 + lax.rem(me + d, 8) for d in (1, 7, 2, 6, 3, 5, 4)]
    across = [lax.rem(me + 8 * d, groups) for d in range(1, 4)]
    for dest in line + across:
        signal(barrier, dest)
    ends = (lax.rem(me, 8) == 7, lax.rem(me, 8) == 0)

    @pl.when(ends[0])
    def _():
        signal(barrier, following)

    @pl.when(ends[1])
    def _():
        signal(barrier, lax.rem(me + groups - 1, groups))

    for one in loads:
        one.start()

    def near_entered():
        place = lax.rem(me, 8)
        pl.semaphore_wait(barrier, 10 + lax.div(place, 7) + lax.div(7 - place, 7))

    def send(src, dst, dest, send_sem, recv_sem):
        return pltpu.make_async_remote_copy(
            src, dst, send_sem, recv_sem, device_id={"tm": dest}, device_id_type=MESH
        )

    def halo(part):
        s, rows = part // 2, pl.ds(part % 2 * 4 * J, 4 * J)
        return send(
            vbuf.at[s, pl.ds(blocks, 2), rows], vbuf.at[s, pl.ds(0, 2), rows],
            following, halo_send.at[part], halo_recv.at[part],
        )

    others = [
        lax.rem(plane + dz, 4) * 8 + lax.rem(column + dy, 4) * 2 + lax.rem(core + dc, 2)
        for dz, dy in FAR_FIRST for dc in (0, 1) if (dz, dy, dc) != (0, 0, 0)
    ]

    def split_taps():
        for jb in range(J // 8):
            t = [taps[pl.ds(jb * 64 + ((k // 8) * 256 + k % 8), 8, stride=8), :] for k in range(TAPS)]
            for i in range(quarter):
                a, b, c, d = t[4 * i:4 * i + 4]
                for place, h in enumerate((a, c, a + c, b, d, b + d, a + b, c + d, (a + b) + (c + d))):
                    tap_sums[jb, place, i] = h

    def fir(first, count, s, jb, slot):
        groups_of_four = count // 4
        keep = xbuf.at[jb % 2]

        def sample(g):
            return vbuf.at[s, (first + g + 16) // 8][pl.ds(jb * 64 + (g + 16) % 8, 8, stride=8), :]

        def run(h, x):
            total = h[0] * x[quarter - 1]
            for i in range(1, quarter):
                total = total + h[i] * x[quarter - 1 - i]
            return total

        def nested(level, even, odd, give):
            h = [[tap_sums[jb, 3 * level + k, i] for i in range(quarter)] for k in range(3)]
            x = [even(n) for n in range(1 - quarter, 0)]
            y = [odd(n) for n in range(-quarter, 0)]
            z = [a + b for a, b in zip(x, y[1:])]
            before = run(h[1], y)
            for n in range(groups_of_four):
                x, y = x[1 - quarter:] + [even(n)], y[1:] + [odd(n)]
                z = z[1 - quarter:] + [x[-1] + y[-1]]
                a, b, ab = run(h[0], x), run(h[1], y), run(h[2], z)
                give(n, a + before, ab - (a + b))
                before = b

        place = pl.ds(s * J + jb * 8, 8)
        def even_samples(n, h):
            value = sample(4 * n + 2 * h)
            keep[0, 2 * n + h + 2 * quarter] = value
            return value

        def odd_samples(n, h):
            value = sample(4 * n + 2 * h + 1)
            keep[1, 2 * n + h + 2 * quarter] = value + keep[0, 2 * n + h + 2 * quarter]
            return value

        def sums(n, h):
            return keep[1, 2 * n + h + 2 * quarter]

        def give_even(n, u, v):
            keep[2, 2 * n], keep[2, 2 * n + 1] = u, v

        carried = []

        def give_odd(n, u, v):
            a, b = keep[2, 2 * n], keep[2, 2 * n + 1]
            ybuf[slot, 4 * n, place, :] = a + carried[-1]
            ybuf[slot, 4 * n + 2, place, :] = b + u
            keep[3, 2 * n], keep[3, 2 * n + 1] = a + u, b + v
            carried.append(v)

        def give_sum(n, u, v):
            ybuf[slot, 4 * n + 1, place, :] = u - keep[3, 2 * n]
            ybuf[slot, 4 * n + 3, place, :] = v - keep[3, 2 * n + 1]

        def start():
            total = None
            for i in range(quarter):
                for k in range(2):
                    term = tap_sums[jb, 3 + k, i] * sample(-1 - 4 * i - 2 * k)
                    total = term if total is None else total + term
            carried.append(total)

        start()
        nested(0, lambda n: even_samples(n, 0), lambda n: even_samples(n, 1), give_even)
        nested(1, lambda n: odd_samples(n, 0), lambda n: odd_samples(n, 1), give_odd)
        nested(2, lambda n: sums(n, 0), lambda n: sums(n, 1), give_sum)

    def first_stage(part, slot):
        cosine, sine = twist[0], twist[1]
        for pair in range(4):
            f = part * 8 + pair * 2
            y = jnp.concatenate([ybuf[slot, f], ybuf[slot, f + 1]], axis=1)
            high, low = split(y)
            o = dot(outer[...], jnp.concatenate([high, low, high], axis=0))
            for h in range(2):
                re, im = o[:J, h * L:(h + 1) * L], o[J:, h * L:(h + 1) * L]
                z = jnp.concatenate([re * cosine + im * sine, im * cosine - re * sine], axis=1)
                place = pl.ds((pair * 2 + h) * J, J)
                zbuf[part, 0, place, :], zbuf[part, 1, place, :] = split(z)

    def second_stage(part, slot):
        high, low = zbuf[part, 0], zbuf[part, 1]
        x = dot(high, inner[0]) + dot(low, inner[0]) + dot(high, inner[1])
        power = x[:, :L] * x[:, :L] + x[:, L:] * x[:, L:]
        for r in range(2):
            p = [power[(4 * r + f) * J:(4 * r + f + 1) * J] for f in range(4)]
            row = (p[0] + p[1]) + (p[2] + p[3])
            moments[0] += row
            moments[1] += (p[0] * p[0] + p[1] * p[1]) + (p[2] * p[2] + p[3] * p[3])
            held[slot, part * 2 + r] = row

    def clean_lanes():
        block = lax.broadcasted_iota(jnp.int32, (groups, L), 0)
        lane = lax.broadcasted_iota(jnp.int32, (groups, L), 1)
        spread_out = jnp.where(lane // 4 == block, 1.0, 0.0)
        clean = jnp.broadcast_to(1.0 - flags[...].astype(F32), (8, groups))
        return dot(clean.astype(BF16), spread_out.astype(BF16))[0:1]

    def finish_rows(slot, side, target):
        clean = moments[2, pl.ds(8, 1), :]
        lane = lax.broadcasted_iota(jnp.int32, (1, L), 1)
        rows, inverse, summed = [], None, None
        for a in range(4):
            row = held[slot, side * 4 + a]
            part = jnp.sum(row, axis=0, keepdims=True) * clean
            one = jnp.broadcast_to(1.0 / jnp.sum(part, axis=1, keepdims=True), (1, L))
            inverse = one if a == 0 else jnp.where(lane % 4 == a, one, inverse)
            summed = part if a == 0 else summed + part
            rows.append(row * float(J * L))
        moments[2, pl.ds(0, 1), :] += summed
        target[...] = owners_first(rows, clean * inverse).reshape(groups, 4, L)

    def in_turn(one, count):
        def some(dests):
            for dest in dests:
                one(dest).start()

        return [functools.partial(some, others[n::count]) for n in range(count)]

    def send_wide(g):
        return in_turn(
            lambda dest: send(wide.at[g, dest], dyn.at[me, pl.ds(1 + 2 * g, 2)], dest, row_send, row_recv), 8
        )

    def send_late():
        return in_turn(lambda dest: send(late.at[dest], dyn.at[me, pl.ds(5, 3)], dest, row_send, row_recv), 8)

    pieces = [(s, jb) for s in range(2) for jb in range(J // 8)]

    def stages(parts, slot):
        order = [functools.partial(first_stage, 0, slot)]
        for part in range(1, parts):
            order.append(functools.partial(first_stage, part, slot))
            order.append(functools.partial(second_stage, part - 1, slot))
        return order + [functools.partial(second_stage, parts - 1, slot)]

    def interleave(*lists):
        keyed = [((n + 0.5) / len(one), k, action) for k, one in enumerate(lists) for n, action in enumerate(one)]
        for _, _, action in sorted(keyed, key=lambda entry: entry[:2]):
            action()

    def filters(first, count, slot):
        return [functools.partial(fir, first, count, s, jb, slot) for s, jb in pieces]

    moments[...] = jnp.zeros_like(moments)

    loads[0].wait()
    split_taps()
    loads[1].wait()
    near_entered()

    @pl.when(me < groups - 1)
    def _():
        for part in range(4):
            halo(part).start()

    for dest in across:
        signal(ready, dest)
    loads[2].wait()
    for action in filters(16, 32, 0)[:4]:
        action()
    loads[3].wait()
    for action in filters(16, 32, 0)[4:]:
        action()
    for piece in range(4, 10):
        loads[piece].wait()
    moments[2, pl.ds(8, 1), :] = clean_lanes()

    def finish(slot, side, target):
        return functools.partial(finish_rows, slot, side, target)

    interleave(filters(48, 32, 1))
    interleave(stages(4, 0))
    interleave(stages(4, 1), [finish(0, side, wide.at[0, :, side]) for side in range(2)])
    interleave(filters(80, 32, 0)[:2])
    pl.semaphore_wait(ready, 3)
    interleave(filters(80, 32, 0)[2:], [finish(1, side, wide.at[1, :, side]) for side in range(2)], send_wide(0))
    interleave(filters(112, 16, 1), send_wide(1))
    interleave(stages(4, 0))
    interleave(stages(2, 1), [finish(0, side, late.at[:, side]) for side in range(2)])
    finish_rows(1, 0, late.at[:, 2])
    interleave(send_late())

    @pl.when(me == 0)
    def _():
        vbuf[:, pl.ds(0, 2)] = jnp.zeros((2, 2, 8 * J, L), F32)

    for part in range(4):
        @pl.when(me > 0)
        def _():
            halo(part).wait_recv()

        interleave(filters(0, 16, 0)[2 * part:2 * part + 2])

    interleave(stages(2, 0))
    finish_rows(0, 0, final.at[:, 0])

    local = jnp.sum(moments[2, pl.ds(0, 1), :], axis=1, keepdims=True)
    last = [moments[0], moments[1], jnp.broadcast_to(local, (J, L)), jnp.zeros((J, L), F32)]
    final[:, 1] = owners_first(last).reshape(groups, 4, L)
    for dest in others:
        send(final.at[dest], got.at[me], dest, fin_send, fin_recv).start()
    got[me] = final[me]
    for g in range(2):
        dyn[me, pl.ds(1 + 2 * g, 2)] = wide[g, me]
    dyn[me, pl.ds(5, 3)] = late[me]

    everyone = pl.ds(0, groups - 1)
    send(final.at[everyone], got.at[everyone], following, fin_send, fin_recv).wait_recv()
    lane = lax.broadcasted_iota(jnp.int32, (1, L), 1)
    own = jnp.sum(jnp.where(lane == 4 * me, moments[2, pl.ds(8, 1), :], 0.0), axis=1, keepdims=True)
    mine[...] = jnp.broadcast_to(own, (1, L))

    units = dyn.at[everyone, pl.ds(1, 7)]
    send(units, units, following, row_send, row_recv).wait()
    send(final.at[everyone], got.at[everyone], following, fin_send, fin_recv).wait_send()

    @pl.when(me < groups - 1)
    def _():
        for part in range(4):
            halo(part).wait_send()


def deliver(count, dyn, got, mine, rows, kurt, spec, kbuf, sbuf, sem):
    later = pltpu.make_async_copy(dyn.at[:, pl.ds(1, 7)], rows.at[:, pl.ds(1, 7)], sem.at[0])
    early = pltpu.make_async_copy(got.at[:, 0], rows.at[:, 0], sem.at[1])
    later.start()
    early.start()
    sums = jnp.sum(got[:, 1], axis=0)
    first, second, group = sums[0:1], sums[1:2], sums[2:3]
    kbuf[...] = (count + 1.0) / (count - 1.0) * (count * second / (first * first) - 1.0)
    sbuf[...] = float(J * L) * mine[...] * first / group
    small = [pltpu.make_async_copy(kbuf, kurt, sem.at[2]), pltpu.make_async_copy(sbuf, spec, sem.at[3])]
    for one in small:
        one.start()
    for one in small:
        one.wait()
    later.wait()
    early.wait()


def body(groups, voltages, taps, flags):
    frames = voltages.shape[1]
    volt = voltages.reshape(2, frames // 8, 8, J, L).transpose(0, 1, 3, 2, 4).reshape(2, frames // 8, 8 * J, L)
    tap = taps.reshape(TAPS // 8, 8, J, L).transpose(0, 2, 1, 3).reshape(TAPS * J, L)
    outer, twist, inner = tables()
    vmem = pl.BlockSpec(memory_space=pltpu.VMEM)
    operands = (volt, tap, flags.reshape(1, groups), jnp.asarray(outer), jnp.asarray(twist), jnp.asarray(inner))
    received = pl.pallas_call(
        functools.partial(kernel, groups, frames),
        out_shape=(
            jax.ShapeDtypeStruct((groups, frames // 16, 4, L), F32),
            jax.ShapeDtypeStruct((groups, 2, 4, L), F32),
            jax.ShapeDtypeStruct((1, L), F32),
        ),
        in_specs=[pl.BlockSpec(memory_space=pltpu.HBM)] * 6,
        out_specs=(vmem, vmem, vmem),
        scratch_shapes=[
            pltpu.VMEM((2, frames // 8 + 2, 8 * J, L), F32),
            pltpu.VMEM((TAPS * J, L), F32),
            pltpu.VMEM((1, groups), jnp.int32),
            pltpu.VMEM(outer.shape, BF16),
            pltpu.VMEM(twist.shape, F32),
            pltpu.VMEM(inner.shape, BF16),
            pltpu.VMEM((J // 8, 9, TAPS // 4, 8, L), F32),
            pltpu.VMEM((2, 4, CHUNK // 2 + TAPS // 2, 8, L), F32),
            pltpu.VMEM((2, CHUNK, 2 * J, L), F32),
            pltpu.VMEM((CHUNK // 8, 2, 8 * J, 2 * L), BF16),
            pltpu.VMEM((2, CHUNK // 4, J, L), F32),
            pltpu.VMEM((2, groups, 2, 4, L), F32),
            pltpu.VMEM((groups, 3, 4, L), F32),
            pltpu.VMEM((groups, 2, 4, L), F32),
            pltpu.VMEM((3, J, L), F32),
            pltpu.SemaphoreType.DMA((10,)),
            pltpu.SemaphoreType.REGULAR,
            pltpu.SemaphoreType.DMA((4,)),
            pltpu.SemaphoreType.DMA((4,)),
        ] + [pltpu.SemaphoreType.DMA] * 4,
        compiler_params=pltpu.CompilerParams(
            collective_id=0, has_side_effects=True, vmem_limit_bytes=40 * 1024 * 1024
        ),
    )(*(pltpu.with_memory_space_constraint(x, pltpu.HBM) for x in operands))
    hbm = pl.BlockSpec(memory_space=pltpu.HBM)
    dyn, kurt, spec = pl.pallas_call(
        functools.partial(deliver, float(frames * groups)),
        out_shape=(
            jax.ShapeDtypeStruct((groups, frames // 16, 4, L), F32),
            jax.ShapeDtypeStruct((1, L), F32),
            jax.ShapeDtypeStruct((1, L), F32),
        ),
        in_specs=[vmem] * 3,
        out_specs=(hbm, hbm, hbm),
        scratch_shapes=[pltpu.VMEM((1, L), F32), pltpu.VMEM((1, L), F32), pltpu.SemaphoreType.DMA((4,))],
        compiler_params=pltpu.CompilerParams(vmem_limit_bytes=4 * 1024 * 1024),
    )(*received)
    return dyn.reshape(groups * frames // 4, L), kurt.reshape(L), spec.reshape(L)


def solution(mesh):
    placed = (P(None, ("stream", "tm"), None), P(), P("stream"))
    return jax.shard_map(
        functools.partial(body, mesh.shape["tm"]),
        mesh=mesh,
        in_specs=placed,
        out_specs=(P("stream", "tm"), P(("stream", "tm")), P(("stream", "tm"))),
        check_vma=False,
    )
```

```python
import functools

import jax
import jax.numpy as jnp
import ml_dtypes
import numpy as np
from jax import lax
from jax.experimental import pallas as pl
from jax.experimental.pallas import tpu as pltpu
from jax.sharding import PartitionSpec as P

J, L = 32, 128
TAPS = 16
CHUNK = 32
FAR_FIRST = sorted(
    ((dz, dy) for dz in range(4) for dy in range(4)), key=lambda d: -(min(d[0], 4 - d[0]) + min(d[1], 4 - d[1]))
)
F32, BF16 = jnp.float32, jnp.bfloat16
MESH = pl.DeviceIdType.MESH


def split_table(table):
    high = table.astype(ml_dtypes.bfloat16)
    low = (table - high.astype(np.float64)).astype(ml_dtypes.bfloat16)
    return high, low


def complex_table(turns, steps):
    angle = 2.0 * np.pi * (turns % steps) / steps
    cosine, sine = np.cos(angle), np.sin(angle)
    return cosine, sine


def tables():
    q, j = np.arange(J)[:, None], np.arange(J)[None, :]
    cosine, sine = complex_table(q * j, J)
    outer = np.block([[cosine, sine], [-sine, cosine]])
    high, low = split_table(outer)
    outer_table = np.concatenate([high, high, low], 1)
    cosine, sine = complex_table(q * np.arange(L)[None, :], J * L)
    twist = np.stack([cosine, sine]).astype(np.float32)
    a, m = np.arange(L)[:, None], np.arange(L)[None, :]
    cosine, sine = complex_table(a * m, L)
    inner = np.block([[cosine, -sine], [sine, cosine]])
    return outer_table, twist, np.stack(split_table(inner))


def split(value):
    high = value.astype(BF16)
    low = (value - high.astype(F32)).astype(BF16)
    return high, low


def dot(a, b):
    return jnp.dot(a, b, preferred_element_type=F32)


def exchange(rows):
    lane = lax.broadcasted_iota(jnp.int32, rows[0].shape, 1)
    rows = list(rows)
    for bit in (2, 1):
        upper = (lane & bit) != 0
        for a in range(4):
            if a & bit:
                continue
            x, y = rows[a], rows[a + bit]
            rows[a] = jnp.where(upper, pltpu.roll(y, bit, 1), x)
            rows[a + bit] = jnp.where(upper, y, pltpu.roll(x, L - bit, 1))
    return rows


def owners_first(rows, scale=None):
    rows = exchange(rows)
    if scale is not None:
        rows = [row * scale for row in rows]
    return jnp.concatenate(rows, axis=0).T


def kernel(
    groups, frames,
    volt, taps_in, flags_in, outer_in, twist_in, inner_in,
    dyn, got, mine,
    vbuf, taps, flags, outer, twist, inner, tap_sums, xbuf, ybuf, zbuf, held, wide, late, final, moments,
    load_sem, ready, halo_send, halo_recv, row_send, row_recv, fin_send, fin_recv,
):
    me = lax.axis_index("tm")
    blocks = frames // 8
    quarter = TAPS // 4
    both = pl.ds(0, 2)
    following = lax.rem(me + 1, groups)

    def load(piece, part, first, count):
        return pltpu.make_async_copy(
            volt.at[part, pl.ds(first, count)], vbuf.at[part, pl.ds(first + 2, count)], load_sem.at[piece]
        )

    loads = [
        pltpu.make_async_copy(taps_in, taps, load_sem.at[0]),
        load(1, both, blocks - 2, 2),
        load(2, 0, 0, 6),
        load(3, 1, 0, 6),
        pltpu.make_async_copy(outer_in, outer, load_sem.at[4]),
        pltpu.make_async_copy(twist_in, twist, load_sem.at[5]),
        pltpu.make_async_copy(inner_in, inner, load_sem.at[6]),
        pltpu.make_async_copy(flags_in, flags, load_sem.at[7]),
        load(8, both, 6, 4),
        load(9, both, 10, 4),
    ]
    def signal(semaphore, dest):
        pl.semaphore_signal(semaphore, 1, device_id={"tm": dest}, device_id_type=MESH)

    barrier = pltpu.get_barrier_semaphore()
    column, core, plane = me // 2 % 4, me % 2, me // 8
    line = [plane * 8 + lax.rem(me + d, 8) for d in (1, 7, 2, 6, 3, 5, 4)]
    across = [lax.rem(me + 8 * d, groups) for d in range(1, 4)]
    for dest in line + across:
        signal(barrier, dest)
    ends = (lax.rem(me, 8) == 7, lax.rem(me, 8) == 0)

    @pl.when(ends[0])
    def _():
        signal(barrier, following)

    @pl.when(ends[1])
    def _():
        signal(barrier, lax.rem(me + groups - 1, groups))

    for one in loads:
        one.start()

    def near_entered():
        place = lax.rem(me, 8)
        pl.semaphore_wait(barrier, 10 + lax.div(place, 7) + lax.div(7 - place, 7))

    def send(src, dst, dest, send_sem, recv_sem):
        return pltpu.make_async_remote_copy(
            src, dst, send_sem, recv_sem, device_id={"tm": dest}, device_id_type=MESH
        )

    def halo(part):
        s, rows = part // 2, pl.ds(part % 2 * 4 * J, 4 * J)
        return send(
            vbuf.at[s, pl.ds(blocks, 2), rows], vbuf.at[s, pl.ds(0, 2), rows],
            following, halo_send.at[part], halo_recv.at[part],
        )

    others = [
        lax.rem(plane + dz, 4) * 8 + lax.rem(column + dy, 4) * 2 + lax.rem(core + dc, 2)
        for dz, dy in FAR_FIRST for dc in (0, 1) if (dz, dy, dc) != (0, 0, 0)
    ]

    def split_taps():
        for jb in range(J // 8):
            t = [taps[pl.ds(jb * 64 + ((k // 8) * 256 + k % 8), 8, stride=8), :] for k in range(TAPS)]
            for i in range(quarter):
                a, b, c, d = t[4 * i:4 * i + 4]
                for place, h in enumerate((a, c, a + c, b, d, b + d, a + b, c + d, (a + b) + (c + d))):
                    tap_sums[jb, place, i] = h

    def fir(first, count, s, jb, slot):
        groups_of_four = count // 4
        keep = xbuf.at[jb % 2]

        def sample(g):
            return vbuf.at[s, (first + g + 16) // 8][pl.ds(jb * 64 + (g + 16) % 8, 8, stride=8), :]

        def run(h, x):
            total = h[0] * x[quarter - 1]
            for i in range(1, quarter):
                total = total + h[i] * x[quarter - 1 - i]
            return total

        def nested(level, even, odd, give):
            h = [[tap_sums[jb, 3 * level + k, i] for i in range(quarter)] for k in range(3)]
            x = [even(n) for n in range(1 - quarter, 0)]
            y = [odd(n) for n in range(-quarter, 0)]
            z = [a + b for a, b in zip(x, y[1:])]
            before = run(h[1], y)
            for n in range(groups_of_four):
                x, y = x[1 - quarter:] + [even(n)], y[1:] + [odd(n)]
                z = z[1 - quarter:] + [x[-1] + y[-1]]
                a, b, ab = run(h[0], x), run(h[1], y), run(h[2], z)
                give(n, a + before, ab - (a + b))
                before = b

        place = pl.ds(s * J + jb * 8, 8)
        def even_samples(n, h):
            value = sample(4 * n + 2 * h)
            keep[0, 2 * n + h + 2 * quarter] = value
            return value

        def odd_samples(n, h):
            value = sample(4 * n + 2 * h + 1)
            keep[1, 2 * n + h + 2 * quarter] = value + keep[0, 2 * n + h + 2 * quarter]
            return value

        def sums(n, h):
            return keep[1, 2 * n + h + 2 * quarter]

        def give_even(n, u, v):
            keep[2, 2 * n], keep[2, 2 * n + 1] = u, v

        carried = []

        def give_odd(n, u, v):
            a, b = keep[2, 2 * n], keep[2, 2 * n + 1]
            ybuf[slot, 4 * n, place, :] = a + carried[-1]
            ybuf[slot, 4 * n + 2, place, :] = b + u
            keep[3, 2 * n], keep[3, 2 * n + 1] = a + u, b + v
            carried.append(v)

        def give_sum(n, u, v):
            ybuf[slot, 4 * n + 1, place, :] = u - keep[3, 2 * n]
            ybuf[slot, 4 * n + 3, place, :] = v - keep[3, 2 * n + 1]

        def start():
            total = None
            for i in range(quarter):
                for k in range(2):
                    term = tap_sums[jb, 3 + k, i] * sample(-1 - 4 * i - 2 * k)
                    total = term if total is None else total + term
            carried.append(total)

        start()
        nested(0, lambda n: even_samples(n, 0), lambda n: even_samples(n, 1), give_even)
        nested(1, lambda n: odd_samples(n, 0), lambda n: odd_samples(n, 1), give_odd)
        nested(2, lambda n: sums(n, 0), lambda n: sums(n, 1), give_sum)

    def first_stage(part, slot):
        cosine, sine = twist[0], twist[1]
        for pair in range(4):
            f = part * 8 + pair * 2
            y = jnp.concatenate([ybuf[slot, f], ybuf[slot, f + 1]], axis=1)
            high, low = split(y)
            o = dot(outer[...], jnp.concatenate([high, low, high], axis=0))
            for h in range(2):
                re, im = o[:J, h * L:(h + 1) * L], o[J:, h * L:(h + 1) * L]
                z = jnp.concatenate([re * cosine + im * sine, im * cosine - re * sine], axis=1)
                place = pl.ds((pair * 2 + h) * J, J)
                zbuf[part, 0, place, :], zbuf[part, 1, place, :] = split(z)

    def second_stage(part, slot):
        high, low = zbuf[part, 0], zbuf[part, 1]
        x = dot(high, inner[0]) + dot(low, inner[0]) + dot(high, inner[1])
        power = x[:, :L] * x[:, :L] + x[:, L:] * x[:, L:]
        for r in range(2):
            p = [power[(4 * r + f) * J:(4 * r + f + 1) * J] for f in range(4)]
            row = (p[0] + p[1]) + (p[2] + p[3])
            moments[0] += row
            moments[1] += (p[0] * p[0] + p[1] * p[1]) + (p[2] * p[2] + p[3] * p[3])
            held[slot, part * 2 + r] = row

    def clean_lanes():
        block = lax.broadcasted_iota(jnp.int32, (groups, L), 0)
        lane = lax.broadcasted_iota(jnp.int32, (groups, L), 1)
        spread_out = jnp.where(lane // 4 == block, 1.0, 0.0)
        clean = jnp.broadcast_to(1.0 - flags[...].astype(F32), (8, groups))
        return dot(clean.astype(BF16), spread_out.astype(BF16))[0:1]

    def finish_rows(slot, side, target):
        clean = moments[2, pl.ds(8, 1), :]
        lane = lax.broadcasted_iota(jnp.int32, (1, L), 1)
        rows, inverse, summed = [], None, None
        for a in range(4):
            row = held[slot, side * 4 + a]
            part = jnp.sum(row, axis=0, keepdims=True) * clean
            one = jnp.broadcast_to(1.0 / jnp.sum(part, axis=1, keepdims=True), (1, L))
            inverse = one if a == 0 else jnp.where(lane % 4 == a, one, inverse)
            summed = part if a == 0 else summed + part
            rows.append(row * float(J * L))
        moments[2, pl.ds(0, 1), :] += summed
        target[...] = owners_first(rows, clean * inverse).reshape(groups, 4, L)

    def in_turn(one, count):
        def some(dests):
            for dest in dests:
                one(dest).start()

        return [functools.partial(some, others[n::count]) for n in range(count)]

    def send_wide(g):
        return in_turn(
            lambda dest: send(wide.at[g, dest], dyn.at[me, pl.ds(1 + 2 * g, 2)], dest, row_send, row_recv), 8
        )

    def send_late():
        return in_turn(lambda dest: send(late.at[dest], dyn.at[me, pl.ds(5, 3)], dest, row_send, row_recv), 8)

    pieces = [(s, jb) for s in range(2) for jb in range(J // 8)]

    def stages(parts, slot):
        order = [functools.partial(first_stage, 0, slot)]
        for part in range(1, parts):
            order.append(functools.partial(first_stage, part, slot))
            order.append(functools.partial(second_stage, part - 1, slot))
        return order + [functools.partial(second_stage, parts - 1, slot)]

    def interleave(*lists):
        keyed = [((n + 0.5) / len(one), k, action) for k, one in enumerate(lists) for n, action in enumerate(one)]
        for _, _, action in sorted(keyed, key=lambda entry: entry[:2]):
            action()

    def filters(first, count, slot):
        return [functools.partial(fir, first, count, s, jb, slot) for s, jb in pieces]

    moments[...] = jnp.zeros_like(moments)

    loads[0].wait()
    split_taps()
    loads[1].wait()
    near_entered()

    @pl.when(me < groups - 1)
    def _():
        for part in range(4):
            halo(part).start()

    for dest in across:
        signal(ready, dest)
    loads[2].wait()
    for action in filters(16, 32, 0)[:4]:
        action()
    loads[3].wait()
    for action in filters(16, 32, 0)[4:]:
        action()
    for piece in range(4, 10):
        loads[piece].wait()
    moments[2, pl.ds(8, 1), :] = clean_lanes()

    def finish(slot, side, target):
        return functools.partial(finish_rows, slot, side, target)

    interleave(filters(48, 32, 1))
    interleave(stages(4, 0))
    interleave(stages(4, 1), [finish(0, side, wide.at[0, :, side]) for side in range(2)])
    interleave(filters(80, 32, 0)[:2])
    pl.semaphore_wait(ready, 3)
    interleave(filters(80, 32, 0)[2:], [finish(1, side, wide.at[1, :, side]) for side in range(2)], send_wide(0))
    interleave(filters(112, 16, 1), send_wide(1))
    interleave(stages(4, 0))
    interleave(stages(2, 1), [finish(0, side, late.at[:, side]) for side in range(2)])
    finish_rows(1, 0, late.at[:, 2])
    interleave(send_late())

    @pl.when(me == 0)
    def _():
        vbuf[:, pl.ds(0, 2)] = jnp.zeros((2, 2, 8 * J, L), F32)

    for part in range(4):
        @pl.when(me > 0)
        def _():
            halo(part).wait_recv()

        interleave(filters(0, 16, 0)[2 * part:2 * part + 2])

    interleave(stages(2, 0))
    finish_rows(0, 0, final.at[:, 0])

    local = jnp.sum(moments[2, pl.ds(0, 1), :], axis=1, keepdims=True)
    nothing = jnp.zeros((J, L), F32)
    last = owners_first([moments[0], moments[1], nothing, nothing])
    place = lax.broadcasted_iota(jnp.int32, last.shape, 0)
    final[:, 1] = jnp.where(place % 4 == 2, local, last).reshape(groups, 4, L)
    for dest in others:
        send(final.at[dest], got.at[me], dest, fin_send, fin_recv).start()
    got[me] = final[me]
    for g in range(2):
        dyn[me, pl.ds(1 + 2 * g, 2)] = wide[g, me]
    dyn[me, pl.ds(5, 3)] = late[me]

    everyone = pl.ds(0, groups - 1)
    send(final.at[everyone], got.at[everyone], following, fin_send, fin_recv).wait_recv()
    lane = lax.broadcasted_iota(jnp.int32, (1, L), 1)
    own = jnp.sum(jnp.where(lane == 4 * me, moments[2, pl.ds(8, 1), :], 0.0), axis=1, keepdims=True)
    mine[...] = jnp.broadcast_to(own, (1, L))

    units = dyn.at[everyone, pl.ds(1, 7)]
    send(units, units, following, row_send, row_recv).wait()
    send(final.at[everyone], got.at[everyone], following, fin_send, fin_recv).wait_send()

    @pl.when(me < groups - 1)
    def _():
        for part in range(4):
            halo(part).wait_send()


def deliver(count, dyn, got, mine, rows, kurt, spec, kbuf, sbuf, sem):
    quarter = dyn.shape[0] // 4
    parts = [pl.ds(n * quarter, quarter) for n in range(4)]
    large = [
        pltpu.make_async_copy(dyn.at[part, pl.ds(1, 7)], rows.at[part, pl.ds(1, 7)], sem.at[n])
        for n, part in enumerate(parts)
    ] + [pltpu.make_async_copy(got.at[:, 0], rows.at[:, 0], sem.at[4])]
    for one in large:
        one.start()
    sums = jnp.sum(got[:, 1], axis=0)
    first, second, group = sums[0:1], sums[1:2], sums[2:3]
    kbuf[...] = (count + 1.0) / (count - 1.0) * (count * second / (first * first) - 1.0)
    sbuf[...] = float(J * L) * mine[...] * first / group
    small = [pltpu.make_async_copy(kbuf, kurt, sem.at[5]), pltpu.make_async_copy(sbuf, spec, sem.at[6])]
    for one in small:
        one.start()
    for one in small + large:
        one.wait()


def body(groups, voltages, taps, flags):
    frames = voltages.shape[1]
    volt = voltages.reshape(2, frames // 8, 8, J, L).transpose(0, 1, 3, 2, 4).reshape(2, frames // 8, 8 * J, L)
    tap = taps.reshape(TAPS // 8, 8, J, L).transpose(0, 2, 1, 3).reshape(TAPS * J, L)
    outer, twist, inner = tables()
    vmem = pl.BlockSpec(memory_space=pltpu.VMEM)
    operands = (volt, tap, flags.reshape(1, groups), jnp.asarray(outer), jnp.asarray(twist), jnp.asarray(inner))
    received = pl.pallas_call(
        functools.partial(kernel, groups, frames),
        out_shape=(
            jax.ShapeDtypeStruct((groups, frames // 16, 4, L), F32),
            jax.ShapeDtypeStruct((groups, 2, 4, L), F32),
            jax.ShapeDtypeStruct((1, L), F32),
        ),
        in_specs=[pl.BlockSpec(memory_space=pltpu.HBM)] * 6,
        out_specs=(vmem, vmem, vmem),
        scratch_shapes=[
            pltpu.VMEM((2, frames // 8 + 2, 8 * J, L), F32),
            pltpu.VMEM((TAPS * J, L), F32),
            pltpu.VMEM((1, groups), jnp.int32),
            pltpu.VMEM(outer.shape, BF16),
            pltpu.VMEM(twist.shape, F32),
            pltpu.VMEM(inner.shape, BF16),
            pltpu.VMEM((J // 8, 9, TAPS // 4, 8, L), F32),
            pltpu.VMEM((2, 4, CHUNK // 2 + TAPS // 2, 8, L), F32),
            pltpu.VMEM((2, CHUNK, 2 * J, L), F32),
            pltpu.VMEM((CHUNK // 8, 2, 8 * J, 2 * L), BF16),
            pltpu.VMEM((2, CHUNK // 4, J, L), F32),
            pltpu.VMEM((2, groups, 2, 4, L), F32),
            pltpu.VMEM((groups, 3, 4, L), F32),
            pltpu.VMEM((groups, 2, 4, L), F32),
            pltpu.VMEM((3, J, L), F32),
            pltpu.SemaphoreType.DMA((10,)),
            pltpu.SemaphoreType.REGULAR,
            pltpu.SemaphoreType.DMA((4,)),
            pltpu.SemaphoreType.DMA((4,)),
        ] + [pltpu.SemaphoreType.DMA] * 4,
        compiler_params=pltpu.CompilerParams(
            collective_id=0, has_side_effects=True, vmem_limit_bytes=40 * 1024 * 1024
        ),
    )(*(pltpu.with_memory_space_constraint(x, pltpu.HBM) for x in operands))
    hbm = pl.BlockSpec(memory_space=pltpu.HBM)
    dyn, kurt, spec = pl.pallas_call(
        functools.partial(deliver, float(frames * groups)),
        out_shape=(
            jax.ShapeDtypeStruct((groups, frames // 16, 4, L), F32),
            jax.ShapeDtypeStruct((1, L), F32),
            jax.ShapeDtypeStruct((1, L), F32),
        ),
        in_specs=[vmem] * 3,
        out_specs=(hbm, hbm, hbm),
        scratch_shapes=[pltpu.VMEM((1, L), F32), pltpu.VMEM((1, L), F32), pltpu.SemaphoreType.DMA((7,))],
        compiler_params=pltpu.CompilerParams(vmem_limit_bytes=4 * 1024 * 1024),
    )(*received)
    return dyn.reshape(groups * frames // 4, L), kurt.reshape(L), spec.reshape(L)


def solution(mesh):
    placed = (P(None, ("stream", "tm"), None), P(), P("stream"))
    return jax.shard_map(
        functools.partial(body, mesh.shape["tm"]),
        mesh=mesh,
        in_specs=placed,
        out_specs=(P("stream", "tm"), P(("stream", "tm")), P(("stream", "tm"))),
        check_vma=False,
    )
```
